128 devices in a mesh: section: 8 (over z, core), rows: 16 (over y, x).
Axes of the slice: x: 4, y: 4, z: 4, core: 2. Of those that a mesh axis runs over, the one named last changes fastest.
Arguments:
- features: bfloat16 [2048, 1536], P('rows'), may hold values from -6 to 6
- ages: int32 [2048], P('rows'), may hold values from 0 to 15
- age_table: bfloat16 [16, 1536], replicated, may hold values from -3 to 3
- returns: float32 [2048], P('rows'), may hold values from -6 to 6
- owners: int32 [2048, 1], P('rows'), may hold values from 0 to 15; in each aligned block of 128 rows (0 to 127, 128 to 255, ...) at most 32 rows name the same one
- slots: int32 [2048], P('rows'), may hold values from 0 to 4095
- norm_gain: float32 [8, 1536], P('section'), may hold values from 0.1 to 1.9
- w_gate: bfloat16 [8, 1536, 8960], P('section', None, 'rows'), may hold values from -0.15625 to 0.15625
- w_up: bfloat16 [8, 1536, 8960], P('section', None, 'rows'), may hold values from -0.15625 to 0.15625
- w_down: bfloat16 [8, 8960, 1536], P('section', 'rows'), may hold values from -0.0625 to 0.0625
- final_gain: float32 [1536], replicated, may hold values from 0.1 to 1.9
- reward_head: float32 [1536], replicated, may hold values from -0.15625 to 0.15625
- old_priority: float32 [65536], P('rows'), may hold values from 0.05 to 2
Outputs:
- rewards: float32 [2048], P(('rows', 'section'))
- weights: float32 [65536], P(('rows', 'section'))
The draws below stay inside these ranges and needn't reach their ends.
Inputs may be any that keep to these rules, and one draw needn't show every extreme that they name: `owners`: among the rows of one device at most 32 name the same owner; in every draw some owner is named by exactly 32 rows of some device.
All inputs are finite; a program needn't handle non-finite values.
Results may differ from the reference program's by a relative error of at most 0.04.
Values may be sent and summed in bfloat16 or wider, within the bound.
A program may use at most 64 MiB of HBM per device.

```python
import math
import jax
import jax.numpy as jnp
import numpy as np
from jax import lax

D = 1536
FF = 8960
AGES = 16
CAP = 32
ROWS_DEV = 128
BUF_DEV = 4096
LAYERS = 8
ROWS = 2048
OWNERS = 16
BUF = 65536


def set_ends(result, own_key, low, high):
    longest = result.shape.index(max(result.shape))
    spots = []
    for shift in (0, 1):
        where = [jax.random.randint(jax.random.fold_in(own_key, axis), (), 0, length) for axis, length in enumerate(result.shape)]
        where[longest] = (where[longest] + shift) % result.shape[longest]
        spots.append(tuple(where))
    return result.at[spots[0]].set(low).at[spots[1]].set(high)


def shard_levels(key, extent, cuts, least, high):
    loudness, own = 1.0, jax.random.fold_in(key, 6)
    for axis_at, parts in cuts:
        steps = jnp.exp(jax.random.uniform(jax.random.fold_in(own, axis_at), (parts,), jnp.float32, least / len(cuts), high / len(cuts)))
        loudness = loudness * jnp.repeat(steps, extent[axis_at] // parts).reshape([-1 if axis == axis_at else 1 for axis in range(len(extent))])
    return loudness


def assign_block(stream_key, own, number, rows, amount, top, reach, slope):
    order = jax.random.permutation(stream_key, amount)
    packed, usual = portions_of(amount, rows * top, reach, slope, True), portions_of(amount, rows * top, reach, slope, False)
    places = jnp.arange(amount)

    def named(lengths, rotation):
        used = int((lengths > 0).sum())
        fixed = max(1, used // 4)
        passed = fixed + (places - fixed + rotation * (used - fixed)) % max(1, amount - fixed)
        return jnp.zeros((amount,), jnp.int32).at[order[jnp.where(places < fixed, places, passed)]].set(jnp.asarray(lengths, jnp.int32))

    lengths = jnp.where(number % 4 == 0, named(packed, number // 4), named(usual, number - number // 4 - 1))
    mixed = jax.random.permutation(jax.random.fold_in(own, 3), amount)
    giver, sink = mixed[0:amount // 2 * 2:2], mixed[1:amount // 2 * 2:2]
    margin = jnp.minimum(lengths[giver] - 1, reach - lengths[sink]) // 2
    margin = jnp.where((giver == order[0]) | (sink == order[0]) | (lengths[sink] == 0), 0, jnp.maximum(margin, 0))
    passed = jax.random.randint(jax.random.fold_in(own, 4), (amount // 2,), 0, 1 << 20) % (margin + 1)
    lengths = lengths.at[giver].add(-passed).at[sink].add(passed)
    items = jnp.searchsorted(jnp.cumsum(lengths), jnp.arange(rows * top), side="right").astype(jnp.int32)
    grid = items.reshape(top, rows).T
    grid = grid[jax.random.permutation(jax.random.fold_in(own, 1), rows)]
    rotation = jax.random.randint(jax.random.fold_in(own, 2), (rows, 1), 0, top)
    return jnp.take_along_axis(grid, (jnp.arange(top)[None, :] + rotation) % top, axis=1)


def portions_of(count, total, reach, skew, full):
    loads = [(1 << 20) // math.isqrt(grade ** skew) + 1 for grade in range(1, count + 1)]
    largest = reach if full else min(reach, max(-(-total // count), total * loads[0] // sum(loads)))
    least = 1 if total - largest >= count - 1 else 0
    counts, surplus = [largest] + [least] * (count - 1), total - largest - least * (count - 1)
    while surplus > 0:
        candidates = [i for i in range(1, count) if counts[i] < largest] or [i for i in range(1, count) if counts[i] < reach]
        whole, budget = sum([loads[i] for i in candidates]), surplus
        for i in candidates:
            more = min(reach - counts[i], max(1, budget * loads[i] // whole), surplus)
            counts[i] = counts[i] + more
            surplus = surplus - more
    return np.array(counts)


def normal_values(key, dims, scale, most, split=(), dtype=jnp.bfloat16):
    result = scale * jax.random.normal(key, dims, jnp.float32)
    if split:
        result = result * shard_levels(key, dims, split, -0.22, 0.18)
    return jnp.clip(result, -most, most).astype(dtype)


def setup_inputs(seed: int = 0) -> dict:
    arg_keys = jax.random.split(jax.random.key(seed), 14)
    features = normal_values(arg_keys[0], (ROWS, D), 1.0, 6.0, ((0, 16),))
    ages = set_ends(jax.random.randint(arg_keys[1], (ROWS,), 0, AGES), jax.random.fold_in(arg_keys[1], 1), 0, AGES - 1).astype(jnp.int32)
    age_table = normal_values(arg_keys[2], (AGES, D), 0.5, 3.0)
    returns = normal_values(arg_keys[3], (ROWS,), 1.0, 6.0, ((0, 16),), jnp.float32)
    owners_keys = jax.random.split(jax.random.fold_in(arg_keys[4], 1), ROWS // ROWS_DEV)
    owners_turns = jax.random.permutation(jax.random.fold_in(arg_keys[4], 3), ROWS // ROWS_DEV)
    owners = jax.vmap(lambda own, number: assign_block(jax.random.fold_in(arg_keys[4], 2), own, number, ROWS_DEV, OWNERS, 1, CAP, 2))(owners_keys, owners_turns).reshape((ROWS, 1))
    slots = set_ends(jax.random.randint(arg_keys[5], (ROWS,), 0, BUF_DEV), jax.random.fold_in(arg_keys[5], 1), 0, BUF_DEV - 1).astype(jnp.int32)
    norm_gain = jnp.clip(1.0 + 0.18 * jax.random.normal(arg_keys[6], (LAYERS, D), jnp.float32), 0.1, 1.9)
    w_gate = normal_values(arg_keys[7], (LAYERS, D, FF), D ** -0.5, 0.15625, ((0, 8), (2, 16)))
    w_up = normal_values(arg_keys[8], (LAYERS, D, FF), D ** -0.5, 0.15625, ((0, 8), (2, 16)))
    w_down = normal_values(arg_keys[9], (LAYERS, FF, D), FF ** -0.5, 0.0625, ((0, 8), (1, 16)))
    final_gain = jnp.clip(1.0 + 0.18 * jax.random.normal(arg_keys[10], (D,), jnp.float32), 0.1, 1.9)
    reward_head = normal_values(arg_keys[11], (D,), D ** -0.5, 0.15625, (), jnp.float32)
    old_priority = jnp.clip(jnp.exp(math.log(2.0) - 3.6888794 * jax.random.uniform(arg_keys[12], (BUF,), jnp.float32) ** shard_levels(arg_keys[12], (BUF,), ((0, 16),), -0.2, 0.2)), 0.05, 2.0)
    return dict(features=features, ages=ages, age_table=age_table, returns=returns, owners=owners, slots=slots, norm_gain=norm_gain, w_gate=w_gate, w_up=w_up, w_down=w_down, final_gain=final_gain, reward_head=reward_head, old_priority=old_priority)


def scaled_norm(values, gain):
    return values * lax.rsqrt(lax.optimization_barrier(jnp.mean(values * values, axis=-1, keepdims=True)) + 1e-06) * gain

def reference(features, ages, age_table, returns, owners, slots, norm_gain, w_gate, w_up, w_down, final_gain, reward_head, old_priority):
    onehot = (ages[:, None] == jnp.arange(AGES)[None, :]).astype(jnp.bfloat16)
    state = (features.astype(jnp.float32) + jnp.dot(onehot, age_table, preferred_element_type=jnp.float32)).astype(jnp.bfloat16)
    for layer in range(LAYERS):
        wide = state.astype(jnp.float32)
        normed = scaled_norm(wide, norm_gain[layer]).astype(jnp.bfloat16)
        gate = jnp.dot(normed, w_gate[layer], preferred_element_type=jnp.float32)
        upper = jnp.dot(normed, w_up[layer], preferred_element_type=jnp.float32)
        hidden = (jax.nn.silu(gate) * upper).astype(jnp.bfloat16)
        state = (wide + jnp.dot(hidden, w_down[layer], preferred_element_type=jnp.float32)).astype(jnp.bfloat16)
    finished = scaled_norm(state.astype(jnp.float32), final_gain)
    rewards = lax.optimization_barrier(jnp.sum(finished * reward_head, axis=-1))
    priority = jnp.exp(0.6 * jnp.log(jnp.abs(rewards - returns) + 0.05))
    target = (owners[:, 0] * BUF_DEV + slots).astype(jnp.int32)
    largest = jax.ops.segment_max(priority, target, num_segments=BUF)
    counted = jax.ops.segment_sum(jnp.ones_like(priority), target, num_segments=BUF)
    refreshed = jnp.where(counted > 0, largest, old_priority)
    weights = refreshed * (BUF / jnp.sum(refreshed))
    return (rewards, weights)
```

```python
import functools

import jax
import jax.numpy as jnp
from jax import lax
from jax.experimental import pallas as pl
from jax.experimental.pallas import tpu as pltpu
from jax.sharding import PartitionSpec as P

MESH = pl.DeviceIdType.MESH
MICRO = 16
GROUP = 8
SPAN = 640


def place(member, half):
    y = member // 2
    return 4 * y + 2 * (member % 2) + (y + half) % 2


def copy_to(src, dst, send, recv, section, rows):
    return pltpu.make_async_remote_copy(
        src_ref=src,
        dst_ref=dst,
        send_sem=send,
        recv_sem=recv,
        device_id={"section": section, "rows": rows},
        device_id_type=MESH,
    )


def take(ref, sem):
    pltpu.make_async_copy(ref, ref, sem).wait()


def model_kernel(
    x0,
    gain_in,
    wg_in,
    wu_in,
    wd_in,
    final_gain,
    head,
    out,
    wg,
    wu,
    wd,
    gain,
    xs,
    ag,
    rs,
    ps,
    hid,
    rew,
    news,
    allrew,
    own_sem,
    w0_send,
    w0_recv,
    w1_send,
    w1_recv,
    x_send,
    x_recv,
    ag_send,
    ag_recv,
    rs_send,
    rs_recv,
    all_send,
    all_recv,
):
    section = lax.axis_index("section")
    rows = lax.axis_index("rows")
    plane, core = section // 2, section % 2
    y, x = rows // 4, rows % 4
    half = (x + y) % 2
    stage = 2 * plane + half
    member = y * 2 + x // 2
    primary = core == half
    sibling = 2 * plane + 1 - core
    later = (stage + 1) % 8
    later_half = later % 2
    later_section = 2 * (later // 2) + core
    width = x0.shape[-1]
    r = x0.shape[1]
    block = GROUP * r

    near = (
        4 * y + (x + 1) % 4,
        4 * y + (x + 3) % 4,
        4 * ((y + 1) % 4) + x,
        4 * ((y + 3) % 4) + x,
    )
    lanes = ((0, 128), (128, 128), (256, 128), (384, 256))
    downs = ((0, 128), (128, 128), (256, 128), (384, 176))

    def own_copies():
        return (
            pltpu.make_async_copy(wg_in, wg.at[:, pl.ds(0, SPAN)], own_sem.at[0]),
            pltpu.make_async_copy(wu_in, wu.at[:, pl.ds(0, SPAN)], own_sem.at[1]),
            pltpu.make_async_copy(wd_in, wd.at[pl.ds(0, SPAN), :], own_sem.at[2]),
            pltpu.make_async_copy(gain_in, gain, own_sem.at[3]),
        )

    def sibling_copies():
        pairs = (
            (wg_in, wg.at[:, pl.ds(0, SPAN)]),
            (wu_in, wu.at[:, pl.ds(0, SPAN)]),
            (wd_in, wd.at[pl.ds(0, SPAN), :]),
            (gain_in, gain),
        )
        return [
            copy_to(src, dst, w0_send.at[i], w0_recv.at[i], sibling, rows)
            for i, (src, dst) in enumerate(pairs)
        ]

    def piece_copies(n, to_section, to_rows, relay):
        at, size = lanes[n]
        d_at, d_size = downs[n]
        g_dst = wg.at[:, pl.ds(SPAN + at, size)]
        u_dst = wu.at[:, pl.ds(SPAN + at, size)]
        d_dst = wd.at[pl.ds(SPAN + d_at, d_size), :]
        sources = (
            (g_dst, u_dst, d_dst)
            if relay
            else (
                wg_in.at[:, pl.ds(at, size)],
                wu_in.at[:, pl.ds(at, size)],
                wd_in.at[pl.ds(d_at, d_size), :],
            )
        )
        return [
            copy_to(src, dst, w1_send.at[i, n], w1_recv.at[i, n], to_section, to_rows)
            for i, (src, dst) in enumerate(zip(sources, (g_dst, u_dst, d_dst)))
        ]

    @pl.when(primary)
    def _():
        for copy in own_copies():
            copy.start()
        for copy in sibling_copies():
            copy.start()

    @pl.when(jnp.logical_not(primary))
    def _():
        for n in range(4):
            for copy in piece_copies(n, section, near[n], False):
                copy.start()

    wd[pl.ds(SPAN + 560, SPAN - 560), :] = jnp.zeros((SPAN - 560, width), jnp.bfloat16)

    def feed():
        return copy_to(x0, xs, x_send, x_recv, section, place(member, 0))

    @pl.when(jnp.logical_and(section == 1, half == 1))
    def _():
        feed().start()

    @pl.when(jnp.logical_and(section == 0, half == 0))
    def _():
        xs[...] = x0[...]

    def summed(m):
        take(rs.at[m], rs_recv.at[m])
        total = rs[m, 0].astype(jnp.float32)
        for i in range(1, GROUP + 1):
            total = total + rs[m, i].astype(jnp.float32)
        return total.astype(jnp.bfloat16)

    def enter(m):
        @pl.when(stage > 0)
        def _():
            xs[m] = summed(m)

        copy_to(
            xs.at[m],
            rs.at[m, GROUP],
            rs_send.at[m],
            rs_recv.at[m],
            later_section,
            place(member, later_half),
        ).start()
        wide = xs[m].astype(jnp.float32)
        mean = jnp.mean(wide * wide, axis=-1, keepdims=True)
        ag[m, member] = (wide * lax.rsqrt(mean + 1e-06) * gain[...]).astype(jnp.bfloat16)
        for step in range(1, GROUP):
            peer = (member + step) % GROUP
            copy_to(
                ag.at[m, member],
                ag.at[m, member],
                ag_send.at[m],
                ag_recv.at[m],
                section,
                place(peer, half),
            ).start()

    def layer(m):
        take(ag.at[m, pl.ds(0, GROUP - 1)], ag_recv.at[m])
        normed = ag[m].reshape(block, width)
        for at in range(0, 2 * SPAN, 256):
            gate = jnp.dot(normed, wg[:, at : at + 256], preferred_element_type=jnp.float32)
            upper = jnp.dot(normed, wu[:, at : at + 256], preferred_element_type=jnp.float32)
            hid[:, at : at + 256] = (gate * jax.nn.sigmoid(gate) * upper).astype(jnp.bfloat16)
        for at in range(0, width, 256):
            part = jnp.dot(hid[...], wd[:, at : at + 256], preferred_element_type=jnp.float32)
            ps[m, :, :, at : at + 256] = part.astype(jnp.bfloat16).reshape(GROUP, r, 256)
        for step in range(GROUP):
            peer = (member + step) % GROUP
            copy_to(
                ps.at[m, peer],
                rs.at[m, member],
                rs_send.at[m],
                rs_recv.at[m],
                later_section,
                place(peer, later_half),
            ).start()

    @pl.when(jnp.logical_and(section == 1, half == 0))
    def _():
        take(xs, x_recv)

    @pl.when(primary)
    def _():
        own_copies()[3].wait()

    @pl.when(jnp.logical_not(primary))
    def _():
        take(gain, w0_recv.at[3])

    @pl.when(stage == 0)
    def _():
        enter(0)

    @pl.when(primary)
    def _():
        for n in range(4):
            for i, copy in enumerate(piece_copies(n, sibling, rows, True)):
                copy.wait_recv()
                copy.start()
        for copy in own_copies()[:3]:
            copy.wait()

    @pl.when(jnp.logical_not(primary))
    def _():
        for copy in sibling_copies()[:3]:
            copy.wait_recv()
        for n in range(4):
            for copy in piece_copies(n, section, near[n], False):
                copy.wait_recv()

    @pl.when(stage > 0)
    def _():
        enter(0)

    def tick(m, carry):
        @pl.when(m + 1 < MICRO)
        def _():
            enter(m + 1)

        layer(m)
        return carry

    lax.fori_loop(0, MICRO, tick, 0)

    def reach(step):
        flat = (section * 16 + rows + step) % 128
        return copy_to(
            news,
            allrew.at[place(member, core)],
            all_send,
            all_recv,
            flat // 16,
            flat % 16,
        )

    @pl.when(stage == 0)
    def _():
        def finish(m, line):
            wide = summed(m).astype(jnp.float32)
            mean = jnp.mean(wide * wide, axis=-1, keepdims=True)
            ready = wide * lax.rsqrt(mean + 1e-06) * final_gain[...]
            value = jnp.sum(ready * head[...], axis=-1, keepdims=True)
            spot = lax.broadcasted_iota(jnp.int32, (r, 128), 0) + m * r
            lane = lax.broadcasted_iota(jnp.int32, (r, 128), 1)
            return line + jnp.where(spot == lane, value, 0.0)

        line = lax.fori_loop(0, MICRO, finish, jnp.zeros((r, 128), jnp.float32))
        line = jnp.broadcast_to(jnp.sum(line, axis=0, keepdims=True), (8, 128))
        news[...] = line
        allrew[place(member, core)] = line

        def send(step, carry):
            reach(step).start()
            return carry

        lax.fori_loop(1, 128, send, 0)
        take(allrew.at[pl.ds(0, 15)], all_recv)

    @pl.when(stage > 0)
    def _():
        take(allrew, all_recv)

    out[...] = allrew[...]

    @pl.when(stage == 0)
    def _():
        def sent(step, carry):
            take(allrew, all_send)
            return carry

        lax.fori_loop(0, 7, sent, 0)
        take(allrew.at[pl.ds(0, 15)], all_send)

    def drained(m, carry):
        take(ag.at[m, pl.ds(0, GROUP - 1)], ag_send.at[m])
        take(rs.at[m], rs_send.at[m])
        return carry

    lax.fori_loop(0, MICRO, drained, 0)

    @pl.when(jnp.logical_and(section == 1, half == 1))
    def _():
        feed().wait_send()

    @pl.when(primary)
    def _():
        for copy in sibling_copies():
            copy.wait_send()
        for n in range(4):
            for copy in piece_copies(n, sibling, rows, True):
                copy.wait_send()

    @pl.when(jnp.logical_not(primary))
    def _():
        for n in range(4):
            for copy in piece_copies(n, section, near[n], False):
                copy.wait_send()


def model(x0, gain, w_gate, w_up, w_down, final_gain, head):
    rows_here, width = x0.shape
    r = rows_here // MICRO
    vmem = pl.BlockSpec(memory_space=pltpu.VMEM)
    hbm = pl.BlockSpec(memory_space=pl.ANY)
    dma = pltpu.SemaphoreType.DMA
    return pl.pallas_call(
        model_kernel,
        out_shape=jax.ShapeDtypeStruct((16, 8, 128), jnp.float32),
        in_specs=[vmem, hbm, hbm, hbm, hbm, vmem, vmem],
        out_specs=vmem,
        scratch_shapes=[
            pltpu.VMEM((width, 2 * SPAN), jnp.bfloat16),
            pltpu.VMEM((width, 2 * SPAN), jnp.bfloat16),
            pltpu.VMEM((2 * SPAN, width), jnp.bfloat16),
            pltpu.VMEM((1, width), jnp.float32),
            pltpu.VMEM((MICRO, r, width), jnp.bfloat16),
            pltpu.VMEM((MICRO, GROUP, r, width), jnp.bfloat16),
            pltpu.VMEM((MICRO, GROUP + 1, r, width), jnp.bfloat16),
            pltpu.VMEM((MICRO, GROUP, r, width), jnp.bfloat16),
            pltpu.VMEM((GROUP * r, 2 * SPAN), jnp.bfloat16),
            pltpu.VMEM((8, 128), jnp.float32),
            pltpu.VMEM((8, 128), jnp.float32),
            pltpu.VMEM((16, 8, 128), jnp.float32),
            dma((4,)),
            dma((4,)),
            dma((4,)),
            dma((3, 4)),
            dma((3, 4)),
            dma,
            dma,
            dma((MICRO,)),
            dma((MICRO,)),
            dma((MICRO,)),
            dma((MICRO,)),
            dma,
            dma,
        ],
        compiler_params=pltpu.CompilerParams(
            has_side_effects=True, vmem_limit_bytes=60 * 1024 * 1024
        ),
        name="reward_model",
    )(x0.reshape(MICRO, r, width), gain, w_gate, w_up, w_down, final_gain, head)


def on_device(
    features,
    ages,
    age_table,
    returns,
    owners,
    slots,
    norm_gain,
    w_gate,
    w_up,
    w_down,
    final_gain,
    reward_head,
    old_priority,
):
    sections = lax.axis_size("section")
    section = lax.axis_index("section")
    groups = lax.axis_size("rows")
    group = lax.axis_index("rows")
    table_size = old_priority.shape[0]
    onehot = (ages[:, None] == jnp.arange(age_table.shape[0])[None, :]).astype(jnp.bfloat16)
    entry = (
        features.astype(jnp.float32)
        + jnp.dot(onehot, age_table, preferred_element_type=jnp.float32)
    ).astype(jnp.bfloat16)
    extra = SPAN - w_gate.shape[2]
    everyone = model(
        entry,
        norm_gain,
        jnp.pad(w_gate[0], ((0, 0), (0, extra))),
        jnp.pad(w_up[0], ((0, 0), (0, extra))),
        jnp.pad(w_down[0], ((0, extra), (0, 0))),
        final_gain[None, :],
        reward_head[None, :],
    )
    rewards = everyone[:, 0, :]
    names = (owners[:, 0] * table_size + slots).astype(jnp.float32)
    told = lax.all_gather(jnp.stack([returns, names]), "rows")
    priority = jnp.exp(0.6 * jnp.log(jnp.abs(rewards - told[:, 0]) + 0.05)).reshape(-1)
    named = told[:, 1].reshape(-1)
    share = table_size // sections
    entries = group * table_size + section * share + jnp.arange(share)
    match = named[:, None] == entries[None, :].astype(jnp.float32)
    best = jnp.max(jnp.where(match, priority[:, None], 0.0), axis=0)
    old = lax.dynamic_slice_in_dim(old_priority, section * share, share, 0)
    refreshed = jnp.where(best > 0.0, best, old)
    total = lax.psum(jnp.sum(refreshed), ("rows", "section"))
    weights = refreshed * (table_size * groups / total)
    part = rewards.shape[1] // sections
    rewards_out = lax.dynamic_slice(rewards, (group, section * part), (1, part))[0]
    return (rewards_out, weights)


def solution(mesh):
    placed = (
        P("rows", None),
        P("rows"),
        P(),
        P("rows"),
        P("rows", None),
        P("rows"),
        P("section", None),
        P("section", None, "rows"),
        P("section", None, "rows"),
        P("section", "rows", None),
        P(),
        P(),
        P("rows"),
    )
    return jax.shard_map(
        on_device,
        mesh=mesh,
        in_specs=placed,
        out_specs=(P(("rows", "section")), P(("rows", "section"))),
        check_vma=False,
    )
```

```python
import functools

import jax
import jax.numpy as jnp
from jax import lax
from jax.experimental import pallas as pl
from jax.experimental.pallas import tpu as pltpu
from jax.sharding import PartitionSpec as P

MESH = pl.DeviceIdType.MESH
MICRO = 16
GROUP = 8
OWN = 560
SPAN = 1152
TABLE = 4096


def place(member, half):
    y = member // 2
    return 4 * y + 2 * (member % 2) + (y + half) % 2


def copy_to(src, dst, send, recv, section, rows):
    return pltpu.make_async_remote_copy(
        src_ref=src,
        dst_ref=dst,
        send_sem=send,
        recv_sem=recv,
        device_id={"section": section, "rows": rows},
        device_id_type=MESH,
    )


FIRST = (((0,), (0,)), ((), ()))


def take(ref, sem):
    pltpu.make_async_copy(ref, ref, sem).wait()


PIECES = ((0, 144), (144, 144), (288, 144), (432, 128))
GATHER_ORDER = ((2, 1), (1, 0), (3, 0), (1, 1), (3, 1), (0, 1), (2, 0))
SCATTER_ORDER = ((2, 0), (2, 1), (1, 1), (3, 1), (1, 0), (3, 0), (0, 0), (0, 1))


def model_kernel(
    features,
    ages,
    age_table,
    returns,
    owners,
    slots,
    gain_in,
    wg_in,
    wu_in,
    wd_in,
    final_gain,
    head,
    old,
    out_rewards,
    out_weights,
    wg_rows,
    wu_rows,
    wg,
    wu,
    wd,
    gain,
    x0,
    xs,
    ag,
    rs,
    ps,
    hid,
    news,
    allrew,
    told,
    sums,
    own_sem,
    w0_send,
    w0_recv,
    w1_send,
    w1_recv,
    x_send,
    x_recv,
    ag_send,
    ag_recv,
    rs_send,
    rs_recv,
    all_send,
    all_recv,
    told_send,
    told_recv,
    sum_send,
    sum_recv,
):
    section = lax.axis_index("section")
    rows = lax.axis_index("rows")
    plane, core = section // 2, section % 2
    y, x = rows // 4, rows % 4
    half = (x + y) % 2
    stage = 2 * plane + half
    member = y * 2 + x // 2
    primary = core == half
    sibling = 2 * plane + 1 - core
    later = (stage + 1) % 8
    later_half = later % 2
    later_section = 2 * (later // 2) + core
    across_section = 2 * ((plane + half + half + 3) % 4) + core
    width = features.shape[-1]
    r = features.shape[0] // MICRO
    block = GROUP * r

    def peer_of(dy, db):
        return 2 * ((y + dy) % 4) + (member + db) % 2

    barrier = pltpu.get_barrier_semaphore()

    def greet(to_section, to_rows):
        pl.semaphore_signal(
            barrier,
            inc=1,
            device_id={"section": to_section, "rows": to_rows},
            device_id_type=MESH,
        )

    for step in range(1, 16):
        greet(section, (rows + step) % 16)
    greet(sibling, rows)
    for k in range(GROUP):
        greet(across_section, place(k, 1 - half))
    pl.semaphore_wait(barrier, 24)

    near = (
        4 * y + (x + 1) % 4,
        4 * y + (x + 3) % 4,
        4 * ((y + 1) % 4) + x,
        4 * ((y + 3) % 4) + x,
    )

    def own_copies():
        return (
            pltpu.make_async_copy(gain_in, gain, own_sem.at[0]),
            pltpu.make_async_copy(wg_in, wg_rows.at[pl.ds(0, OWN)], own_sem.at[1]),
            pltpu.make_async_copy(wu_in, wu_rows.at[pl.ds(0, OWN)], own_sem.at[2]),
            pltpu.make_async_copy(wd_in, wd.at[pl.ds(0, OWN)], own_sem.at[3]),
        )

    def sibling_copies():
        pairs = (
            (gain_in, gain),
            (wg_in, wg_rows.at[pl.ds(0, OWN)]),
            (wu_in, wu_rows.at[pl.ds(0, OWN)]),
            (wd_in, wd.at[pl.ds(0, OWN)]),
        )
        return [
            copy_to(src, dst, w0_send.at[i], w0_recv.at[i], sibling, rows)
            for i, (src, dst) in enumerate(pairs)
        ]

    def piece_copies(n, to_section, to_rows, relay):
        at, size = PIECES[n]
        targets = [ref.at[pl.ds(OWN + at, size)] for ref in (wg_rows, wu_rows, wd)]
        sources = targets if relay else [ref.at[pl.ds(at, size)] for ref in (wg_in, wu_in, wd_in)]
        return [
            copy_to(src, dst, w1_send.at[i, n], w1_recv.at[i, n], to_section, to_rows)
            for i, (src, dst) in enumerate(zip(sources, targets))
        ]

    def feed(part):
        return copy_to(
            x0.at[pl.ds(4 * part, 4)],
            xs.at[pl.ds(4 * part, 4)],
            x_send.at[part],
            x_recv.at[part],
            section,
            place(member, 0),
        )

    feeding = jnp.logical_and(section == 1, half == 1)

    @pl.when(jnp.logical_and(plane == 0, primary))
    def _():
        number = age_table.shape[0]
        level = lax.broadcasted_iota(jnp.int32, (number, features.shape[0]), 0)
        onehot = (level == ages[...]).astype(jnp.float32).astype(jnp.bfloat16)
        aged = lax.dot_general(onehot, age_table[...], FIRST, preferred_element_type=jnp.float32)
        entry = (features[...].astype(jnp.float32) + aged).reshape(MICRO, r, width)
        x0[...] = entry.astype(jnp.bfloat16)

        @pl.when(half == 0)
        def _():
            xs[...] = x0[...]

    @pl.when(feeding)
    def _():
        for part in range(4):
            feed(part).start()

    @pl.when(primary)
    def _():
        for copy in own_copies():
            copy.start()
        for copy in sibling_copies():
            copy.start()

    @pl.when(jnp.logical_not(primary))
    def _():
        for i in range(3):
            for n in range(4):
                piece_copies(n, section, near[n], False)[i].start()

    tail = pl.ds(2 * OWN, SPAN - 2 * OWN)
    for ref in (wg_rows, wu_rows, wd):
        ref[tail, :] = jnp.zeros((SPAN - 2 * OWN, width), jnp.bfloat16)

    def enter(m):
        @pl.when(jnp.logical_and(jnp.logical_and(section == 1, half == 0), m % 4 == 0))
        def _():
            take(xs.at[pl.ds(m, 4)], x_recv.at[m // 4])

        @pl.when(stage > 0)
        def _():
            xs[m] = summed(m)

        wide = xs[m].astype(jnp.float32)
        mean = jnp.mean(wide * wide, axis=-1, keepdims=True)
        ag[m, member] = (wide * lax.rsqrt(mean + 1e-06) * gain[...]).astype(jnp.bfloat16)
        for dy, db in GATHER_ORDER:
            copy_to(
                ag.at[m, member],
                ag.at[m, member],
                ag_send.at[m],
                ag_recv.at[m],
                section,
                place(peer_of(dy, db), half),
            ).start()
        copy_to(
            xs.at[m],
            rs.at[m, GROUP],
            rs_send.at[m],
            rs_recv.at[m],
            later_section,
            place(member, later_half),
        ).start()

    def summed(m):
        take(rs.at[m], rs_recv.at[m])
        total = rs[m, 0].astype(jnp.float32)
        for i in range(1, GROUP + 1):
            total = total + rs[m, i].astype(jnp.float32)
        return total.astype(jnp.bfloat16)

    def layer(m):
        take(ag.at[m, pl.ds(0, GROUP - 1)], ag_recv.at[m])
        normed = ag[m].reshape(block, width)
        for at in range(0, SPAN, 256):
            size = min(256, SPAN - at)
            gate = jnp.dot(normed, wg[:, at : at + size], preferred_element_type=jnp.float32)
            upper = jnp.dot(normed, wu[:, at : at + size], preferred_element_type=jnp.float32)
            hid[:, at : at + size] = (gate * jax.nn.sigmoid(gate) * upper).astype(jnp.bfloat16)
        for at in range(0, width, 256):
            part = jnp.dot(hid[...], wd[:, at : at + 256], preferred_element_type=jnp.float32)
            ps[m, :, :, at : at + 256] = part.astype(jnp.bfloat16).reshape(GROUP, r, 256)
        for dy, db in SCATTER_ORDER:
            peer = peer_of(dy, db)
            copy_to(
                ps.at[m, peer],
                rs.at[m, member],
                rs_send.at[m],
                rs_recv.at[m],
                later_section,
                place(peer, later_half),
            ).start()

    def turned(first, last):
        def turn(i, carry):
            at = pl.multiple_of(i * 128, 128)
            wg[:, pl.ds(at, 128)] = wg_rows[pl.ds(at, 128), :].T
            wu[:, pl.ds(at, 128)] = wu_rows[pl.ds(at, 128), :].T
            return carry

        lax.fori_loop(first, last, turn, 0)

    @pl.when(primary)
    def _():
        own_copies()[0].wait()

    @pl.when(jnp.logical_not(primary))
    def _():
        sibling_copies()[0].wait_recv()

    ahead = jnp.where(stage == 0, 3, 1)

    def early(m, carry):
        enter(m)
        return carry

    @pl.when(stage == 0)
    def _():
        lax.fori_loop(0, ahead, early, 0)

    news[...] = (owners[...] * TABLE + slots[...]).astype(jnp.float32)
    told[rows, 0] = returns[...]
    told[rows, 1] = news[...]
    for step in range(1, 16):
        copy_to(
            told.at[rows],
            told.at[rows],
            told_send,
            told_recv,
            section,
            (rows + step) % 16,
        ).start()

    @pl.when(primary)
    def _():
        for copy in own_copies()[1:]:
            copy.wait()

    @pl.when(jnp.logical_not(primary))
    def _():
        for copy in sibling_copies()[1:]:
            copy.wait_recv()

    turned(0, 4)
    for n in range(4):

        @pl.when(primary)
        def _():
            for copy in piece_copies(n, sibling, rows, True):
                copy.wait_recv()
                copy.start()

        @pl.when(jnp.logical_not(primary))
        def _():
            for copy in piece_copies(n, section, near[n], False):
                copy.wait_recv()

        turned(4 + n, 5 + n if n < 3 else 9)

    @pl.when(stage > 0)
    def _():
        lax.fori_loop(0, ahead, early, 0)

    def tick(m, carry):
        @pl.when(m + ahead < MICRO)
        def _():
            enter(m + ahead)

        layer(m)
        return carry

    lax.fori_loop(0, MICRO, tick, 0)
    take(told.at[pl.ds(0, 15)], told_recv)

    def flat(step):
        target = (section * 16 + rows + step) % 128
        return target // 16, target % 16

    shard = place(member, core)

    @pl.when(stage == 0)
    def _():
        def finish(m, line):
            wide = summed(m).astype(jnp.float32)
            mean = jnp.mean(wide * wide, axis=-1, keepdims=True)
            ready = wide * lax.rsqrt(mean + 1e-06) * final_gain[...]
            value = jnp.sum(ready * head[...], axis=-1, keepdims=True)
            spot = lax.broadcasted_iota(jnp.int32, (r, 128), 0) + m * r
            lane = lax.broadcasted_iota(jnp.int32, (r, 128), 1)
            return line + jnp.where(spot == lane, value, 0.0)

        line = lax.fori_loop(0, MICRO, finish, jnp.zeros((r, 128), jnp.float32))
        allrew[shard] = jnp.sum(line, axis=0, keepdims=True)

        def send(step, carry):
            to_section, to_rows = flat(step)
            copy_to(
                allrew.at[shard], allrew.at[shard], all_send, all_recv, to_section, to_rows
            ).start()
            return carry

        lax.fori_loop(1, 128, send, 0)
        take(allrew.at[pl.ds(0, 15)], all_recv)

    @pl.when(stage > 0)
    def _():
        take(allrew, all_recv)

    out_rewards[...] = allrew[rows]
    share = TABLE // 8
    lane = lax.broadcasted_iota(jnp.int32, (8, 128), 1)
    sub = lax.broadcasted_iota(jnp.int32, (8, 128), 0)
    priority, named = [], []
    for j in range(16):
        gap = jnp.abs(allrew[j] - told[j, 0]) + 0.05
        priority.append(jnp.broadcast_to(jnp.exp(0.6 * jnp.log(gap)), (8, 128)))
        named.append(jnp.broadcast_to(told[j, 1], (8, 128)))
    first = rows * TABLE + section * share
    lines = []
    for q in range(share // 128):
        line = jnp.zeros((8, 128), jnp.float32)
        for g in range(16):
            entry = (first + q * 128 + g * 8 + sub).astype(jnp.float32)
            best = jnp.zeros((8, 128), jnp.float32)
            for j in range(16):
                best = jnp.maximum(best, jnp.where(named[j] == entry, priority[j], 0.0))
            value = jnp.max(best, axis=1, keepdims=True)
            line = line + jnp.where(lane == g * 8 + sub, value, 0.0)
        lines.append(jnp.sum(line, axis=0, keepdims=True))
    kept = old[pl.ds(pl.multiple_of(8 * (section // 2), 8), 8), :]
    total = jnp.zeros((1, 128), jnp.float32)
    for q in range(share // 128):
        before = jnp.where(section % 2 == 0, kept[q : q + 1], kept[q + 4 : q + 5])
        lines[q] = jnp.where(lines[q] > 0.0, lines[q], before)
        total = total + lines[q]
    mine = section * 16 + rows
    sums[mine] = jnp.broadcast_to(jnp.sum(total, axis=1, keepdims=True), (1, 128))

    def send_sum(step, carry):
        to_section, to_rows = flat(step)
        copy_to(
            sums.at[mine], sums.at[mine], sum_send, sum_recv, to_section, to_rows
        ).start()
        return carry

    lax.fori_loop(1, 128, send_sum, 0)

    @pl.when(stage == 0)
    def _():
        take(sums.at[pl.ds(0, 127)], all_send)

    def drained(m, carry):
        take(ag.at[m, pl.ds(0, GROUP - 1)], ag_send.at[m])
        take(rs.at[m], rs_send.at[m])
        return carry

    lax.fori_loop(0, MICRO, drained, 0)
    take(told.at[pl.ds(0, 15)], told_send)

    @pl.when(feeding)
    def _():
        for part in range(4):
            feed(part).wait_send()

    @pl.when(primary)
    def _():
        for copy in sibling_copies():
            copy.wait_send()
        for n in range(4):
            for copy in piece_copies(n, sibling, rows, True):
                copy.wait_send()

    @pl.when(jnp.logical_not(primary))
    def _():
        for n in range(4):
            for copy in piece_copies(n, section, near[n], False):
                copy.wait_send()

    take(sums.at[pl.ds(0, 127)], sum_recv)
    whole = jnp.sum(sums[...], axis=0)
    for q in range(share // 128):
        out_weights[q : q + 1, :] = lines[q] * (float(16 * TABLE) / whole)
    take(sums.at[pl.ds(0, 127)], sum_send)


def on_device(
    features,
    ages,
    age_table,
    returns,
    owners,
    slots,
    norm_gain,
    w_gate,
    w_up,
    w_down,
    final_gain,
    reward_head,
    old_priority,
):
    sections = lax.axis_size("section")
    section = lax.axis_index("section")
    rows_here, width = features.shape
    r = rows_here // MICRO
    vmem = pl.BlockSpec(memory_space=pltpu.VMEM)
    hbm = pl.BlockSpec(memory_space=pl.ANY)
    dma = pltpu.SemaphoreType.DMA
    half, single = jnp.bfloat16, jnp.float32
    line, weights = pl.pallas_call(
        model_kernel,
        out_shape=[
            jax.ShapeDtypeStruct((1, rows_here), single),
            jax.ShapeDtypeStruct((TABLE // sections // 128, 128), single),
        ],
        in_specs=[vmem] * 6 + [hbm] * 4 + [vmem] * 3,
        out_specs=[vmem] * 2,
        scratch_shapes=[
            pltpu.VMEM((SPAN, width), half),
            pltpu.VMEM((SPAN, width), half),
            pltpu.VMEM((width, SPAN), half),
            pltpu.VMEM((width, SPAN), half),
            pltpu.VMEM((SPAN, width), half),
            pltpu.VMEM((1, width), single),
            pltpu.VMEM((MICRO, r, width), half),
            pltpu.VMEM((MICRO, r, width), half),
            pltpu.VMEM((MICRO, GROUP, r, width), half),
            pltpu.VMEM((MICRO, GROUP + 1, r, width), half),
            pltpu.VMEM((MICRO, GROUP, r, width), half),
            pltpu.VMEM((GROUP * r, SPAN), half),
            pltpu.VMEM((1, 128), single),
            pltpu.VMEM((16, 1, 128), single),
            pltpu.VMEM((16, 2, 1, 128), single),
            pltpu.VMEM((128, 1, 128), single),
            dma((4,)),
            dma((4,)),
            dma((4,)),
            dma((3, 4)),
            dma((3, 4)),
            dma((4,)),
            dma((4,)),
            dma((MICRO,)),
            dma((MICRO,)),
            dma((MICRO,)),
            dma((MICRO,)),
            dma,
            dma,
            dma,
            dma,
            dma,
            dma,
        ],
        compiler_params=pltpu.CompilerParams(
            collective_id=0, has_side_effects=True, vmem_limit_bytes=60 * 1024 * 1024
        ),
        name="reward_model",
    )(
        features,
        ages.reshape(1, rows_here),
        age_table,
        returns.reshape(1, rows_here),
        owners.reshape(1, rows_here),
        slots.reshape(1, rows_here),
        norm_gain,
        w_gate[0].T,
        w_up[0].T,
        w_down[0],
        final_gain.reshape(1, width),
        reward_head.reshape(1, width),
        old_priority.reshape(TABLE // 128, 128),
    )
    part = rows_here // sections
    rewards = lax.dynamic_slice_in_dim(line[0], section * part, part, 0)
    return (rewards, weights.reshape(-1))


def solution(mesh):
    placed = (
        P("rows", None),
        P("rows"),
        P(),
        P("rows"),
        P("rows", None),
        P("rows"),
        P("section", None),
        P("section", None, "rows"),
        P("section", None, "rows"),
        P("section", "rows", None),
        P(),
        P(),
        P("rows"),
    )
    return jax.shard_map(
        on_device,
        mesh=mesh,
        in_specs=placed,
        out_specs=(P(("rows", "section")), P(("rows", "section"))),
        check_vma=False,
    )
```

```python
import functools

import jax
import jax.numpy as jnp
from jax import lax
from jax.experimental import pallas as pl
from jax.experimental.pallas import tpu as pltpu
from jax.sharding import PartitionSpec as P

MESH = pl.DeviceIdType.MESH
MICRO = 16
GROUP = 8
OWN = 560
SPAN = 1152
TABLE = 4096
EARLY = 13


def place(member, half):
    y = member // 2
    return 4 * y + 2 * (member % 2) + (y + half) % 2


def copy_to(src, dst, send, recv, section, rows):
    return pltpu.make_async_remote_copy(
        src_ref=src,
        dst_ref=dst,
        send_sem=send,
        recv_sem=recv,
        device_id={"section": section, "rows": rows},
        device_id_type=MESH,
    )


FIRST = (((0,), (0,)), ((), ()))


def take(ref, sem):
    pltpu.make_async_copy(ref, ref, sem).wait()


PIECES = ((0, 144), (144, 144), (288, 144), (432, 128))
GATHER_ORDER = ((2, 1), (1, 0), (3, 0), (1, 1), (3, 1), (0, 1), (2, 0))
SCATTER_ORDER = ((2, 0), (2, 1), (1, 1), (3, 1), (1, 0), (3, 0), (0, 0), (0, 1))


def model_kernel(
    features,
    ages,
    age_table,
    returns,
    owners,
    slots,
    gain_in,
    wg_in,
    wu_in,
    wd_in,
    final_gain,
    head,
    old,
    out_rewards,
    out_weights,
    wg_rows,
    wu_rows,
    wg,
    wu,
    wd,
    gain,
    x0,
    xs,
    ag,
    rs,
    ps,
    hid,
    news,
    allrew,
    told,
    sums,
    cols,
    shares,
    bests,
    own_sem,
    w0_send,
    w0_recv,
    w1_send,
    w1_recv,
    x_send,
    x_recv,
    ag_send,
    ag_recv,
    rs_send,
    rs_recv,
    all_send,
    all_recv,
    told_send,
    told_recv,
    sum_send,
    sum_recv,
):
    section = lax.axis_index("section")
    rows = lax.axis_index("rows")
    plane, core = section // 2, section % 2
    y, x = rows // 4, rows % 4
    half = (x + y) % 2
    stage = 2 * plane + half
    member = y * 2 + x // 2
    primary = core == half
    sibling = 2 * plane + 1 - core
    last = stage == 7
    later_half = 1 - half
    later_section = jnp.where(last | (half == 0), section, (section + 2) % 8)
    base = jnp.where(last, MICRO, 0)
    across_section = 2 * ((plane + half + half + 3) % 4) + core
    width = features.shape[-1]
    r = features.shape[0] // MICRO
    block = GROUP * r

    def peer_of(dy, db):
        return 2 * ((y + dy) % 4) + (member + db) % 2

    barrier = pltpu.get_barrier_semaphore()

    def greet(to_section, to_rows):
        pl.semaphore_signal(
            barrier,
            inc=1,
            device_id={"section": to_section, "rows": to_rows},
            device_id_type=MESH,
        )

    for step in range(1, 16):
        greet(section, (rows + step) % 16)
    greet(sibling, rows)
    for k in range(GROUP):
        greet(across_section, place(k, 1 - half))
    pl.semaphore_wait(barrier, 24)

    near = (
        4 * y + (x + 1) % 4,
        4 * y + (x + 3) % 4,
        4 * ((y + 1) % 4) + x,
        4 * ((y + 3) % 4) + x,
    )

    def own_copies():
        return (
            pltpu.make_async_copy(gain_in, gain, own_sem.at[0]),
            pltpu.make_async_copy(wg_in, wg_rows.at[pl.ds(0, OWN)], own_sem.at[1]),
            pltpu.make_async_copy(wu_in, wu_rows.at[pl.ds(0, OWN)], own_sem.at[2]),
            pltpu.make_async_copy(wd_in, wd.at[pl.ds(0, OWN)], own_sem.at[3]),
        )

    def sibling_copies():
        pairs = (
            (gain_in, gain),
            (wg_in, wg_rows.at[pl.ds(0, OWN)]),
            (wu_in, wu_rows.at[pl.ds(0, OWN)]),
            (wd_in, wd.at[pl.ds(0, OWN)]),
        )
        return [
            copy_to(src, dst, w0_send.at[i], w0_recv.at[i], sibling, rows)
            for i, (src, dst) in enumerate(pairs)
        ]

    def piece_copies(n, to_section, to_rows, relay):
        at, size = PIECES[n]
        targets = [ref.at[pl.ds(OWN + at, size)] for ref in (wg_rows, wu_rows, wd)]
        sources = targets if relay else [ref.at[pl.ds(at, size)] for ref in (wg_in, wu_in, wd_in)]
        return [
            copy_to(src, dst, w1_send.at[i, n], w1_recv.at[i, n], to_section, to_rows)
            for i, (src, dst) in enumerate(zip(sources, targets))
        ]

    gather_rows = [place(peer_of(dy, db), half) for dy, db in GATHER_ORDER]
    scatter_peers = [peer_of(dy, db) for dy, db in SCATTER_ORDER]
    scatter_rows = [place(peer, later_half) for peer in scatter_peers]

    def feed(part):
        return copy_to(
            x0.at[pl.ds(4 * part, 4)],
            xs.at[pl.ds(4 * part, 4)],
            x_send.at[part],
            x_recv.at[part],
            1,
            place(member, 0),
        )

    feeding = jnp.logical_and(section == 7, half == 1)
    entering = jnp.logical_and(section == 0, half == 0)

    @pl.when(jnp.logical_or(entering, feeding))
    def _():
        number = age_table.shape[0]
        level = lax.broadcasted_iota(jnp.int32, (number, features.shape[0]), 0)
        onehot = (level == ages[...]).astype(jnp.float32).astype(jnp.bfloat16)
        aged = lax.dot_general(onehot, age_table[...], FIRST, preferred_element_type=jnp.float32)
        entry = (features[...].astype(jnp.float32) + aged).reshape(MICRO, r, width)
        x0[...] = entry.astype(jnp.bfloat16)

        @pl.when(entering)
        def _():
            xs[...] = x0[...]

    @pl.when(feeding)
    def _():
        for part in range(4):
            feed(part).start()

    @pl.when(primary)
    def _():
        for copy in own_copies():
            copy.start()
        for copy in sibling_copies():
            copy.start()

    @pl.when(jnp.logical_not(primary))
    def _():
        for i in range(3):
            for n in range(4):
                piece_copies(n, section, near[n], False)[i].start()

    tail = pl.ds(2 * OWN, SPAN - 2 * OWN)
    for ref in (wg_rows, wu_rows, wd):
        ref[tail, :] = jnp.zeros((SPAN - 2 * OWN, width), jnp.bfloat16)

    def enter(m):
        @pl.when(jnp.logical_and(jnp.logical_and(section == 1, half == 0), m % 4 == 0))
        def _():
            take(xs.at[pl.ds(m, 4)], x_recv.at[m // 4])

        @pl.when(stage > 0)
        def _():
            xs[m] = summed(m)

        wide = xs[m].astype(jnp.float32)
        mean = jnp.mean(wide * wide, axis=-1, keepdims=True)
        ag[m, member] = (wide * lax.rsqrt(mean + 1e-06) * gain[...]).astype(jnp.bfloat16)
        for to_rows in gather_rows:
            copy_to(
                ag.at[m, member], ag.at[m, member], ag_send.at[m], ag_recv.at[m], section, to_rows
            ).start()

    def summed(m):
        take(rs.at[m], rs_recv.at[m])
        total = rs[m, 0].astype(jnp.float32)
        for i in range(1, GROUP):
            total = total + rs[m, i].astype(jnp.float32)
        return total.astype(jnp.bfloat16)

    def layer(m):
        take(ag.at[m, pl.ds(0, GROUP - 1)], ag_recv.at[m])
        normed = ag[m].reshape(block, width)
        for at in range(0, SPAN, 256):
            size = min(256, SPAN - at)
            gate = jnp.dot(normed, wg[:, at : at + size], preferred_element_type=jnp.float32)
            upper = jnp.dot(normed, wu[:, at : at + size], preferred_element_type=jnp.float32)
            hid[:, at : at + size] = (gate * jax.nn.sigmoid(gate) * upper).astype(jnp.bfloat16)
        ours = lax.broadcasted_iota(jnp.int32, (GROUP, r, 256), 0) == member
        for at in range(0, width, 256):
            part = jnp.dot(hid[...], wd[:, at : at + 256], preferred_element_type=jnp.float32)
            kept = xs[m, :, at : at + 256].astype(jnp.float32)[None]
            part = part.reshape(GROUP, r, 256) + jnp.where(ours, kept, 0.0)
            ps[m, :, :, at : at + 256] = part.astype(jnp.bfloat16)
            if at + 256 in (width // 2, width):
                span = pl.ds(at + 256 - width // 2, width // 2)
                for peer, to_rows in zip(scatter_peers, scatter_rows):
                    copy_to(
                        ps.at[m, peer, :, span],
                        rs.at[base + m, member, :, span],
                        rs_send.at[m],
                        rs_recv.at[base + m],
                        later_section,
                        to_rows,
                    ).start()

    def turned(source, target):
        def turn(i, carry):
            at = pl.multiple_of(i * 128, 128)
            target[:, pl.ds(at, 128)] = source[pl.ds(at, 128), :].T
            return carry

        lax.fori_loop(0, SPAN // 128, turn, 0)

    @pl.when(primary)
    def _():
        own_copies()[0].wait()

    @pl.when(jnp.logical_not(primary))
    def _():
        sibling_copies()[0].wait_recv()

    ahead = jnp.where(stage == 0, 3, 1)

    def early(m, carry):
        enter(m)
        return carry

    @pl.when(stage == 0)
    def _():
        lax.fori_loop(0, ahead, early, 0)

    news[...] = (owners[...] * TABLE + slots[...]).astype(jnp.float32)
    told[rows, 0] = returns[...]
    told[rows, 1] = news[...]
    for step in range(1, 16):
        copy_to(
            told.at[rows],
            told.at[rows],
            told_send,
            told_recv,
            section,
            (rows + step) % 16,
        ).start()

    @pl.when(primary)
    def _():
        for copy in own_copies()[1:]:
            copy.wait()

    @pl.when(jnp.logical_not(primary))
    def _():
        for copy in sibling_copies()[1:]:
            copy.wait_recv()

    for i in range(3):
        for n in range(4):

            @pl.when(primary)
            def _():
                copy = piece_copies(n, sibling, rows, True)[i]
                copy.wait_recv()
                copy.start()

            @pl.when(jnp.logical_not(primary))
            def _():
                piece_copies(n, section, near[n], False)[i].wait_recv()

        if i < 2:
            turned((wg_rows, wu_rows)[i], (wg, wu)[i])

    share = TABLE // 8
    parts = share // 128
    lane = lax.broadcasted_iota(jnp.int32, (8, 128), 1)
    sub = lax.broadcasted_iota(jnp.int32, (8, 128), 0)
    first = rows * TABLE + section * share
    mine = section * 16 + rows
    side = section % 2

    def before(q):
        near_old = old[pl.ds(pl.multiple_of(8 * (section // 2), 8), 8), :]
        return jnp.where(side == 0, near_old[q : q + 1], near_old[q + parts : q + parts + 1])

    def lines():
        wide = [jnp.broadcast_to(told[j, 1], (8, 128)) for j in range(16)]
        return wide + [(first + q * 128 + lane).astype(jnp.float32) for q in range(parts)]

    def column(line, m):
        picked = jnp.where(lane == m * r + sub, jnp.broadcast_to(line, (8, 128)), 0.0)
        return jnp.broadcast_to(jnp.sum(picked, axis=1, keepdims=True), (8, 128))

    def prepare():
        take(told.at[pl.ds(0, 15)], told_recv)
        names = lines()

        def count(j, totals):
            for m in range(MICRO):
                col = column(told[j, 1], m)
                cols[j, m] = col
                totals = [t + jnp.where(col == name, 1.0, 0.0) for t, name in zip(totals, names)]
            return totals

        zeros = [jnp.zeros((8, 128), jnp.float32)] * len(names)
        totals = lax.fori_loop(0, 16, count, zeros)
        counts = [jnp.sum(t, axis=0, keepdims=True) for t in totals]
        for j in range(16):
            shares[j] = 1.0 / counts[j]
        rest = jnp.zeros((1, 128), jnp.float32)
        for q in range(parts):
            rest = rest + jnp.where(counts[16 + q] > 0.0, 0.0, before(q))
        sums[mine] = jnp.broadcast_to(jnp.sum(rest, axis=1, keepdims=True), (1, 128))

    @pl.when(stage > 3)
    def _():
        prepare()

    @pl.when(stage > 0)
    def _():
        lax.fori_loop(0, ahead, early, 0)

    def tick(m, carry):
        @pl.when(m + ahead < MICRO)
        def _():
            enter(m + ahead)

        layer(m)
        return carry

    lax.fori_loop(0, MICRO, tick, 0)

    @pl.when(stage < 4)
    def _():
        prepare()

    shard = place(member, core)
    final = stage == 6

    def everyone(ref, send, recv):
        def send_one(step, carry):
            target = lax.rem(mine + step, 128)
            copy_to(ref, ref, send, recv, lax.div(target, 16), lax.rem(target, 16)).start()
            return carry

        lax.fori_loop(1, 128, send_one, 0)

    def finish(m, line):
        wide = summed(MICRO + m).astype(jnp.float32)
        mean = jnp.mean(wide * wide, axis=-1, keepdims=True)
        ready = wide * lax.rsqrt(mean + 1e-06) * final_gain[...].reshape(1, width)
        value = jnp.sum(ready * head[...].reshape(1, width), axis=-1, keepdims=True)
        return line + jnp.where(lane == m * r + sub, value, 0.0)

    def share_rewards(turn, start, stop):
        @pl.when(final)
        def _():
            line = lax.fori_loop(start, stop, finish, jnp.zeros((r, 128), jnp.float32))
            allrew[turn, shard] = jnp.sum(line, axis=0, keepdims=True)
            everyone(allrew.at[turn, shard], all_send.at[turn], all_recv.at[turn])

    def await_rewards(turn):
        @pl.when(final)
        def _():
            take(allrew.at[turn, pl.ds(0, 15)], all_recv.at[turn])

        @pl.when(jnp.logical_not(final))
        def _():
            take(allrew.at[turn], all_recv.at[turn])

    def priority(turn, j):
        gap = jnp.abs(allrew[turn, j] - told[j, 0]) + 0.05
        return jnp.exp(0.6 * jnp.log(gap))

    def largest(best, names, line, j, m):
        col, value = cols[j, m], column(line, m)
        return [jnp.maximum(b, jnp.where(col == n, value, 0.0)) for b, n in zip(best, names)]

    share_rewards(0, 0, EARLY)
    await_rewards(0)
    everyone(sums.at[mine], sum_send, sum_recv)
    names = lines()

    def first_round(j, best):
        line = priority(0, j)
        for m in range(EARLY):
            best = largest(best, names, line, j, m)
        return best

    best = lax.fori_loop(0, 16, first_round, [jnp.zeros((8, 128), jnp.float32)] * len(names))
    for i, b in enumerate(best):
        bests[i] = b
    share_rewards(1, EARLY, MICRO)

    def drained(m, carry):
        take(ag.at[m, pl.ds(0, GROUP - 1)], ag_send.at[m])
        take(rs.at[m], rs_send.at[m])
        return carry

    lax.fori_loop(0, MICRO, drained, 0)
    take(told.at[pl.ds(0, 15)], told_send)

    @pl.when(feeding)
    def _():
        for part in range(4):
            feed(part).wait_send()

    @pl.when(primary)
    def _():
        for copy in sibling_copies():
            copy.wait_send()
        for n in range(4):
            for copy in piece_copies(n, sibling, rows, True):
                copy.wait_send()

    @pl.when(jnp.logical_not(primary))
    def _():
        for n in range(4):
            for copy in piece_copies(n, section, near[n], False):
                copy.wait_send()

    take(sums.at[pl.ds(0, 127)], sum_send)
    take(sums.at[pl.ds(0, 127)], sum_recv)
    whole = jnp.sum(sums[...], axis=0)

    await_rewards(1)
    names = lines()
    best = [bests[i] for i in range(len(names))]
    for j in range(16):
        line = priority(1, j)
        for m in range(EARLY, MICRO):
            best = largest(best, names, line, j, m)
    best = [jnp.max(b, axis=0, keepdims=True) for b in best]
    named = jnp.zeros((1, 128), jnp.float32)
    for j in range(16):
        named = named + best[j] * shares[j]
    whole = whole + jnp.sum(named, axis=1, keepdims=True)
    for q in range(parts):
        fresh = jnp.where(best[16 + q] > 0.0, best[16 + q], before(q))
        out_weights[q : q + 1, :] = fresh * (float(16 * TABLE) / whole)
    spots = lax.broadcasted_iota(jnp.int32, (1, 128), 1)
    out_rewards[...] = jnp.where(spots < EARLY * r, allrew[0, rows], allrew[1, rows])

    @pl.when(final)
    def _():
        for turn in range(2):
            take(sums.at[pl.ds(0, 127)], all_send.at[turn])


def on_device(
    features,
    ages,
    age_table,
    returns,
    owners,
    slots,
    norm_gain,
    w_gate,
    w_up,
    w_down,
    final_gain,
    reward_head,
    old_priority,
):
    sections = lax.axis_size("section")
    section = lax.axis_index("section")
    rows_here, width = features.shape
    r = rows_here // MICRO
    vmem = pl.BlockSpec(memory_space=pltpu.VMEM)
    hbm = pl.BlockSpec(memory_space=pl.ANY)
    dma = pltpu.SemaphoreType.DMA
    half, single = jnp.bfloat16, jnp.float32
    line, weights = pl.pallas_call(
        model_kernel,
        out_shape=[
            jax.ShapeDtypeStruct((1, rows_here), single),
            jax.ShapeDtypeStruct((TABLE // sections // 128, 128), single),
        ],
        in_specs=[vmem] * 6 + [hbm] * 4 + [vmem] * 3,
        out_specs=[vmem] * 2,
        scratch_shapes=[
            pltpu.VMEM((SPAN, width), half),
            pltpu.VMEM((SPAN, width), half),
            pltpu.VMEM((width, SPAN), half),
            pltpu.VMEM((width, SPAN), half),
            pltpu.VMEM((SPAN, width), half),
            pltpu.VMEM((1, width), single),
            pltpu.VMEM((MICRO, r, width), half),
            pltpu.VMEM((MICRO, r, width), half),
            pltpu.VMEM((MICRO, GROUP, r, width), half),
            pltpu.VMEM((2 * MICRO, GROUP, r, width), half),
            pltpu.VMEM((MICRO, GROUP, r, width), half),
            pltpu.VMEM((GROUP * r, SPAN), half),
            pltpu.VMEM((1, 128), single),
            pltpu.VMEM((2, 16, 1, 128), single),
            pltpu.VMEM((16, 2, 1, 128), single),
            pltpu.VMEM((128, 1, 128), single),
            pltpu.VMEM((16, MICRO, 8, 128), single),
            pltpu.VMEM((16, 1, 128), single),
            pltpu.VMEM((16 + TABLE // sections // 128, 8, 128), single),
            dma((4,)),
            dma((4,)),
            dma((4,)),
            dma((3, 4)),
            dma((3, 4)),
            dma((4,)),
            dma((4,)),
            dma((MICRO,)),
            dma((MICRO,)),
            dma((MICRO,)),
            dma((2 * MICRO,)),
            dma((2,)),
            dma((2,)),
            dma,
            dma,
            dma,
            dma,
        ],
        compiler_params=pltpu.CompilerParams(
            collective_id=0, has_side_effects=True, vmem_limit_bytes=60 * 1024 * 1024
        ),
        name="reward_model",
    )(
        features,
        ages.reshape(1, rows_here),
        age_table,
        returns.reshape(1, rows_here),
        owners.reshape(1, rows_here),
        slots.reshape(1, rows_here),
        norm_gain,
        w_gate[0].T,
        w_up[0].T,
        w_down[0],
        final_gain,
        reward_head,
        old_priority.reshape(TABLE // 128, 128),
    )
    part = rows_here // sections
    rewards = lax.dynamic_slice_in_dim(line[0], section * part, part, 0)
    return (rewards, weights.reshape(-1))


def solution(mesh):
    placed = (
        P("rows", None),
        P("rows"),
        P(),
        P("rows"),
        P("rows", None),
        P("rows"),
        P("section", None),
        P("section", None, "rows"),
        P("section", None, "rows"),
        P("section", "rows", None),
        P(),
        P(),
        P("rows"),
    )
    return jax.shard_map(
        on_device,
        mesh=mesh,
        in_specs=placed,
        out_specs=(P(("rows", "section")), P(("rows", "section"))),
        check_vma=False,
    )
```

```python
import functools

import jax
import jax.numpy as jnp
from jax import lax
from jax.experimental import pallas as pl
from jax.experimental.pallas import tpu as pltpu
from jax.sharding import PartitionSpec as P

MESH = pl.DeviceIdType.MESH
MICRO = 16
GROUP = 8
OWN = 560
SPAN = 1152
TABLE = 4096
EARLY = 11


def place(member, half):
    y = member // 2
    return 4 * y + 2 * (member % 2) + (y + half) % 2


def copy_to(src, dst, send, recv, section, rows):
    return pltpu.make_async_remote_copy(
        src_ref=src,
        dst_ref=dst,
        send_sem=send,
        recv_sem=recv,
        device_id={"section": section, "rows": rows},
        device_id_type=MESH,
    )


FIRST = (((0,), (0,)), ((), ()))


def take(ref, sem):
    pltpu.make_async_copy(ref, ref, sem).wait()


PIECES = ((0, 144), (144, 144), (288, 144), (432, 128))
GATHER_ORDER = ((2, 1), (1, 0), (3, 0), (1, 1), (3, 1), (0, 1), (2, 0))
SCATTER_ORDER = ((2, 0), (2, 1), (1, 1), (3, 1), (1, 0), (3, 0), (0, 0), (0, 1))


def model_kernel(
    features,
    ages,
    age_table,
    returns,
    owners,
    slots,
    gain_in,
    wg_in,
    wu_in,
    wd_in,
    final_gain,
    head,
    old,
    out_rewards,
    out_weights,
    wg_rows,
    wu_rows,
    wg,
    wu,
    wd,
    gain,
    x0,
    xs,
    ag,
    rs,
    ps,
    hid,
    news,
    allrew,
    told,
    sums,
    cols,
    shares,
    bests,
    given,
    own_sem,
    w0_send,
    w0_recv,
    w1_send,
    w1_recv,
    x_send,
    x_recv,
    ag_send,
    ag_recv,
    rs_send,
    rs_recv,
    all_send,
    all_recv,
    told_send,
    told_recv,
    sum_send,
    sum_recv,
):
    section = lax.axis_index("section")
    rows = lax.axis_index("rows")
    plane, core = section // 2, section % 2
    y, x = rows // 4, rows % 4
    half = (x + y) % 2
    stage = 2 * plane + half
    member = y * 2 + x // 2
    primary = core == half
    sibling = 2 * plane + 1 - core
    last = stage == 7
    later_half = 1 - half
    later_section = jnp.where(half == 0, section, (section + 2) % 8)
    base = jnp.where(last, MICRO, 0)
    across_section = 2 * ((plane + half + half + 3) % 4) + core
    width = features.shape[-1]
    r = features.shape[0] // MICRO
    block = GROUP * r

    def peer_of(dy, db):
        return 2 * ((y + dy) % 4) + (member + db) % 2

    barrier = pltpu.get_barrier_semaphore()

    def greet(to_section, to_rows):
        pl.semaphore_signal(
            barrier,
            inc=1,
            device_id={"section": to_section, "rows": to_rows},
            device_id_type=MESH,
        )

    for step in range(1, 16):
        greet(section, (rows + step) % 16)
    greet(sibling, rows)
    for k in range(GROUP):
        greet(across_section, place(k, 1 - half))
    near = (
        4 * y + (x + 1) % 4,
        4 * y + (x + 3) % 4,
        4 * ((y + 1) % 4) + x,
        4 * ((y + 3) % 4) + x,
    )

    def own_copies():
        return (
            pltpu.make_async_copy(gain_in, gain, own_sem.at[0]),
            pltpu.make_async_copy(wg_in, wg_rows.at[pl.ds(0, OWN)], own_sem.at[1]),
            pltpu.make_async_copy(wu_in, wu_rows.at[pl.ds(0, OWN)], own_sem.at[2]),
            pltpu.make_async_copy(wd_in, wd.at[pl.ds(0, OWN)], own_sem.at[3]),
        )

    def other_copies():
        return [
            pltpu.make_async_copy(src, given.at[i], own_sem.at[i + 1])
            for i, src in enumerate((wg_in, wu_in, wd_in))
        ]

    def sibling_copies():
        pairs = (
            (gain, gain),
            (wg_rows.at[pl.ds(0, OWN)], wg_rows.at[pl.ds(0, OWN)]),
            (wu_rows.at[pl.ds(0, OWN)], wu_rows.at[pl.ds(0, OWN)]),
            (wd.at[pl.ds(0, OWN)], wd.at[pl.ds(0, OWN)]),
        )
        return [
            copy_to(src, dst, w0_send.at[i], w0_recv.at[i], sibling, rows)
            for i, (src, dst) in enumerate(pairs)
        ]

    def piece_copies(n, to_section, to_rows, relay):
        at, size = PIECES[n]
        targets = [ref.at[pl.ds(OWN + at, size)] for ref in (wg_rows, wu_rows, wd)]
        sources = targets if relay else [given.at[i, pl.ds(at, size)] for i in range(3)]
        return [
            copy_to(src, dst, w1_send.at[i, n], w1_recv.at[i, n], to_section, to_rows)
            for i, (src, dst) in enumerate(zip(sources, targets))
        ]

    gather_rows = [place(peer_of(dy, db), half) for dy, db in GATHER_ORDER]
    scatter_peers = [peer_of(dy, db) for dy, db in SCATTER_ORDER]
    scatter_rows = [place(peer, later_half) for peer in scatter_peers]

    def feed(part):
        return copy_to(
            x0.at[pl.ds(4 * part, 4)],
            xs.at[pl.ds(4 * part, 4)],
            x_send.at[part],
            x_recv.at[part],
            1,
            place(member, 0),
        )

    feeding = jnp.logical_and(section == 7, half == 1)
    entering = jnp.logical_and(section == 0, half == 0)

    @pl.when(primary)
    def _():
        for copy in own_copies():
            copy.start()

    @pl.when(jnp.logical_not(primary))
    def _():
        for copy in other_copies():
            copy.start()

    @pl.when(jnp.logical_or(entering, feeding))
    def _():
        number = age_table.shape[0]
        level = lax.broadcasted_iota(jnp.int32, (number, features.shape[0]), 0)
        onehot = (level == ages[...]).astype(jnp.float32).astype(jnp.bfloat16)
        aged = lax.dot_general(onehot, age_table[...], FIRST, preferred_element_type=jnp.float32)
        entry = (features[...].astype(jnp.float32) + aged).reshape(MICRO, r, width)
        x0[...] = entry.astype(jnp.bfloat16)

        @pl.when(entering)
        def _():
            xs[...] = x0[...]

    tail = pl.ds(2 * OWN, SPAN - 2 * OWN)
    for ref in (wg_rows, wu_rows, wd):
        ref[tail, :] = jnp.zeros((SPAN - 2 * OWN, width), jnp.bfloat16)
    news[...] = (owners[...] * TABLE + slots[...]).astype(jnp.float32)
    told[rows, 0] = returns[...]
    told[rows, 1] = news[...]

    pl.semaphore_wait(barrier, 24)

    @pl.when(jnp.logical_not(primary))
    def _():
        for i, copy in enumerate(other_copies()):
            copy.wait()
            for n in range(4):
                piece_copies(n, section, near[n], False)[i].start()

    @pl.when(feeding)
    def _():
        for part in range(4):
            feed(part).start()

    @pl.when(primary)
    def _():
        for own, copy in zip(own_copies(), sibling_copies()):
            own.wait()
            copy.start()

    def enter(m):
        @pl.when(jnp.logical_and(jnp.logical_and(section == 1, half == 0), m % 4 == 0))
        def _():
            take(xs.at[pl.ds(m, 4)], x_recv.at[m // 4])

        @pl.when(stage > 0)
        def _():
            xs[m] = summed(m)

        wide = xs[m].astype(jnp.float32)
        mean = jnp.mean(wide * wide, axis=-1, keepdims=True)
        ag[m, member] = (wide * lax.rsqrt(mean + 1e-06) * gain[...]).astype(jnp.bfloat16)
        for to_rows in gather_rows:
            copy_to(
                ag.at[m, member], ag.at[m, member], ag_send.at[m], ag_recv.at[m], section, to_rows
            ).start()

    def summed(m):
        take(rs.at[m], rs_recv.at[m])
        total = rs[m, 0].astype(jnp.float32)
        for i in range(1, GROUP):
            total = total + rs[m, i].astype(jnp.float32)
        return total.astype(jnp.bfloat16)

    def layer(m):
        take(ag.at[m, pl.ds(0, GROUP - 1)], ag_recv.at[m])
        normed = ag[m].reshape(block, width)
        for at in range(0, SPAN, 256):
            size = min(256, SPAN - at)
            gate = jnp.dot(normed, wg[:, at : at + size], preferred_element_type=jnp.float32)
            upper = jnp.dot(normed, wu[:, at : at + size], preferred_element_type=jnp.float32)
            hid[:, at : at + size] = (gate * jax.nn.sigmoid(gate) * upper).astype(jnp.bfloat16)
        to_section = jnp.where(last & (m >= EARLY), section, later_section)
        ours = lax.broadcasted_iota(jnp.int32, (GROUP, r, 256), 0) == member
        for at in range(0, width, 256):
            part = jnp.dot(hid[...], wd[:, at : at + 256], preferred_element_type=jnp.float32)
            kept = xs[m, :, at : at + 256].astype(jnp.float32)[None]
            part = part.reshape(GROUP, r, 256) + jnp.where(ours, kept, 0.0)
            ps[m, :, :, at : at + 256] = part.astype(jnp.bfloat16)
            if at + 256 in (width // 2, width):
                span = pl.ds(at + 256 - width // 2, width // 2)
                for peer, to_rows in zip(scatter_peers, scatter_rows):
                    copy_to(
                        ps.at[m, peer, :, span],
                        rs.at[base + m, member, :, span],
                        rs_send.at[m],
                        rs_recv.at[base + m],
                        to_section,
                        to_rows,
                    ).start()

    def turned(source, target):
        def turn(i, carry):
            at = pl.multiple_of(i * 128, 128)
            target[:, pl.ds(at, 128)] = source[pl.ds(at, 128), :].T
            return carry

        lax.fori_loop(0, SPAN // 128, turn, 0)

    @pl.when(jnp.logical_not(primary))
    def _():
        sibling_copies()[0].wait_recv()

    begun = jnp.where(stage == 0, 1, 0)

    def early(m, carry):
        enter(m)
        return carry

    lax.fori_loop(0, begun, early, 0)

    for step in range(1, 16):
        copy_to(
            told.at[rows],
            told.at[rows],
            told_send,
            told_recv,
            section,
            (rows + step) % 16,
        ).start()

    @pl.when(jnp.logical_not(primary))
    def _():
        for copy in sibling_copies()[1:]:
            copy.wait_recv()

    for i in range(3):
        for n in range(4):

            @pl.when(primary)
            def _():
                copy = piece_copies(n, sibling, rows, True)[i]
                copy.wait_recv()
                copy.start()

            @pl.when(jnp.logical_not(primary))
            def _():
                piece_copies(n, section, near[n], False)[i].wait_recv()

        if i < 2:
            turned((wg_rows, wu_rows)[i], (wg, wu)[i])

    share = TABLE // 8
    parts = share // 128
    lane = lax.broadcasted_iota(jnp.int32, (8, 128), 1)
    sub = lax.broadcasted_iota(jnp.int32, (8, 128), 0)
    first = rows * TABLE + section * share
    mine = section * 16 + rows
    side = section % 2

    def before(q):
        near_old = old[pl.ds(pl.multiple_of(8 * (section // 2), 8), 8), :]
        return jnp.where(side == 0, near_old[q : q + 1], near_old[q + parts : q + parts + 1])

    def lines():
        wide = [jnp.broadcast_to(told[j, 1], (8, 128)) for j in range(16)]
        return wide + [(first + q * 128 + lane).astype(jnp.float32) for q in range(parts)]

    def column(line, m):
        picked = jnp.where(lane == m * r + sub, jnp.broadcast_to(line, (8, 128)), 0.0)
        return jnp.broadcast_to(jnp.sum(picked, axis=1, keepdims=True), (8, 128))

    def prepare():
        take(told.at[pl.ds(0, 15)], told_recv)
        names = lines()

        def count(j, totals):
            for m in range(MICRO):
                col = column(told[j, 1], m)
                cols[j, m] = col
                totals = [t + jnp.where(col == name, 1.0, 0.0) for t, name in zip(totals, names)]
            return totals

        zeros = [jnp.zeros((8, 128), jnp.float32)] * len(names)
        totals = lax.fori_loop(0, 16, count, zeros)
        counts = [jnp.sum(t, axis=0, keepdims=True) for t in totals]
        for j in range(16):
            shares[j] = 1.0 / counts[j]
        rest = jnp.zeros((1, 128), jnp.float32)
        for q in range(parts):
            rest = rest + jnp.where(counts[16 + q] > 0.0, 0.0, before(q))
        sums[mine] = jnp.broadcast_to(jnp.sum(rest, axis=1, keepdims=True), (1, 128))

    @pl.when(stage > 3)
    def _():
        prepare()

    def tick(m, carry):
        start = jnp.maximum(m + jnp.where(m > 0, 1, 0), begun)
        stop = jnp.minimum(m + 2, MICRO)
        lax.fori_loop(start, stop, early, 0)
        layer(m)
        return carry

    lax.fori_loop(0, MICRO, tick, 0)

    @pl.when(stage < 4)
    def _():
        prepare()

    shard = place(member, core)
    finals = (stage == 0, stage == 6)

    def everyone(ref, send, recv):
        targets = [2 * ((plane + away) % 4) + side for away in (2, 1, 3, 0) for side in (1 - core, core)]

        def send_row(step, carry):
            to_rows = lax.rem(rows + step, 16)
            for to_section in targets:
                copy_to(ref, ref, send, recv, to_section, to_rows).start()
            return carry

        lax.fori_loop(1, 16, send_row, 0)
        for to_section in targets[:-1]:
            copy_to(ref, ref, send, recv, to_section, rows).start()

    def finish(m, line):
        wide = summed(MICRO + m).astype(jnp.float32)
        mean = jnp.mean(wide * wide, axis=-1, keepdims=True)
        ready = wide * lax.rsqrt(mean + 1e-06) * final_gain[...].reshape(1, width)
        value = jnp.sum(ready * head[...].reshape(1, width), axis=-1, keepdims=True)
        return line + jnp.where(lane == m * r + sub, value, 0.0)

    def share_rewards(turn, start, stop):
        @pl.when(finals[turn])
        def _():
            line = lax.fori_loop(start, stop, finish, jnp.zeros((r, 128), jnp.float32))
            allrew[turn, shard] = jnp.sum(line, axis=0, keepdims=True)
            everyone(allrew.at[turn, shard], all_send.at[turn], all_recv.at[turn])

    def await_rewards(turn):
        @pl.when(finals[turn])
        def _():
            take(allrew.at[turn, pl.ds(0, 15)], all_recv.at[turn])

        @pl.when(jnp.logical_not(finals[turn]))
        def _():
            take(allrew.at[turn], all_recv.at[turn])

    def priority(turn, j):
        gap = jnp.abs(allrew[turn, j] - told[j, 0]) + 0.05
        return jnp.exp(0.6 * jnp.log(gap))

    def largest(best, names, line, j, m):
        col, value = cols[j, m], column(line, m)
        return [jnp.maximum(b, jnp.where(col == n, value, 0.0)) for b, n in zip(best, names)]

    share_rewards(0, 0, EARLY)
    await_rewards(0)
    everyone(sums.at[mine], sum_send, sum_recv)
    names = lines()

    def first_round(j, best):
        line = priority(0, j)
        for m in range(EARLY):
            best = largest(best, names, line, j, m)
        return best

    best = lax.fori_loop(0, 16, first_round, [jnp.zeros((8, 128), jnp.float32)] * len(names))
    for i, b in enumerate(best):
        bests[i] = b
    share_rewards(1, EARLY, MICRO)

    def drained(m, carry):
        take(ag.at[m, pl.ds(0, GROUP - 1)], ag_send.at[m])
        take(rs.at[m], rs_send.at[m])
        return carry

    lax.fori_loop(0, MICRO, drained, 0)
    take(told.at[pl.ds(0, 15)], told_send)

    @pl.when(feeding)
    def _():
        for part in range(4):
            feed(part).wait_send()

    @pl.when(primary)
    def _():
        for copy in sibling_copies():
            copy.wait_send()
        for n in range(4):
            for copy in piece_copies(n, sibling, rows, True):
                copy.wait_send()

    @pl.when(jnp.logical_not(primary))
    def _():
        for n in range(4):
            for copy in piece_copies(n, section, near[n], False):
                copy.wait_send()

    take(sums.at[pl.ds(0, 127)], sum_send)
    take(sums.at[pl.ds(0, 127)], sum_recv)
    whole = jnp.sum(sums[...], axis=0)

    await_rewards(1)
    names = lines()
    best = [bests[i] for i in range(len(names))]
    for j in range(16):
        line = priority(1, j)
        for m in range(EARLY, MICRO):
            best = largest(best, names, line, j, m)
    best = [jnp.max(b, axis=0, keepdims=True) for b in best]
    named = jnp.zeros((1, 128), jnp.float32)
    for j in range(16):
        named = named + best[j] * shares[j]
    whole = whole + jnp.sum(named, axis=1, keepdims=True)
    for q in range(parts):
        fresh = jnp.where(best[16 + q] > 0.0, best[16 + q], before(q))
        out_weights[q : q + 1, :] = fresh * (float(16 * TABLE) / whole)
    spots = lax.broadcasted_iota(jnp.int32, (1, 128), 1)
    out_rewards[...] = jnp.where(spots < EARLY * r, allrew[0, rows], allrew[1, rows])

    for turn in range(2):

        @pl.when(finals[turn])
        def _():
            take(sums.at[pl.ds(0, 127)], all_send.at[turn])


def on_device(
    features,
    ages,
    age_table,
    returns,
    owners,
    slots,
    norm_gain,
    w_gate,
    w_up,
    w_down,
    final_gain,
    reward_head,
    old_priority,
):
    sections = lax.axis_size("section")
    section = lax.axis_index("section")
    rows_here, width = features.shape
    r = rows_here // MICRO
    vmem = pl.BlockSpec(memory_space=pltpu.VMEM)
    hbm = pl.BlockSpec(memory_space=pl.ANY)
    dma = pltpu.SemaphoreType.DMA
    half, single = jnp.bfloat16, jnp.float32
    line, weights = pl.pallas_call(
        model_kernel,
        out_shape=[
            jax.ShapeDtypeStruct((1, rows_here), single),
            jax.ShapeDtypeStruct((TABLE // sections // 128, 128), single),
        ],
        in_specs=[vmem] * 6 + [hbm] * 4 + [vmem] * 3,
        out_specs=[vmem] * 2,
        scratch_shapes=[
            pltpu.VMEM((SPAN, width), half),
            pltpu.VMEM((SPAN, width), half),
            pltpu.VMEM((width, SPAN), half),
            pltpu.VMEM((width, SPAN), half),
            pltpu.VMEM((SPAN, width), half),
            pltpu.VMEM((1, width), single),
            pltpu.VMEM((MICRO, r, width), half),
            pltpu.VMEM((MICRO, r, width), half),
            pltpu.VMEM((MICRO, GROUP, r, width), half),
            pltpu.VMEM((2 * MICRO, GROUP, r, width), half),
            pltpu.VMEM((MICRO, GROUP, r, width), half),
            pltpu.VMEM((GROUP * r, SPAN), half),
            pltpu.VMEM((1, 128), single),
            pltpu.VMEM((2, 16, 1, 128), single),
            pltpu.VMEM((16, 2, 1, 128), single),
            pltpu.VMEM((128, 1, 128), single),
            pltpu.VMEM((16, MICRO, 8, 128), single),
            pltpu.VMEM((16, 1, 128), single),
            pltpu.VMEM((16 + TABLE // sections // 128, 8, 128), single),
            pltpu.VMEM((3, OWN, width), half),
            dma((4,)),
            dma((4,)),
            dma((4,)),
            dma((3, 4)),
            dma((3, 4)),
            dma((4,)),
            dma((4,)),
            dma((MICRO,)),
            dma((MICRO,)),
            dma((MICRO,)),
            dma((2 * MICRO,)),
            dma((2,)),
            dma((2,)),
            dma,
            dma,
            dma,
            dma,
        ],
        compiler_params=pltpu.CompilerParams(
            collective_id=0, has_side_effects=True, vmem_limit_bytes=60 * 1024 * 1024
        ),
        name="reward_model",
    )(
        features,
        ages.reshape(1, rows_here),
        age_table,
        returns.reshape(1, rows_here),
        owners.reshape(1, rows_here),
        slots.reshape(1, rows_here),
        norm_gain,
        w_gate[0].T,
        w_up[0].T,
        w_down[0],
        final_gain,
        reward_head,
        old_priority.reshape(TABLE // 128, 128),
    )
    part = rows_here // sections

    def hand_over(line_ref, weights_ref, rewards_out, weights_out):
        turned = pltpu.roll(line_ref[...], (rows_here - section_of() * part) % rows_here, 1)
        rewards_out[...] = turned[:, :part]
        weights_out[...] = weights_ref[...]

    def section_of():
        return lax.axis_index("section")

    rewards, weights = pl.pallas_call(
        hand_over,
        out_shape=[
            jax.ShapeDtypeStruct((1, part), single),
            jax.ShapeDtypeStruct(weights.shape, single),
        ],
        in_specs=[vmem] * 2,
        out_specs=[vmem] * 2,
        name="hand_over",
    )(line, weights)
    return (rewards.reshape(-1), weights.reshape(-1))


def solution(mesh):
    placed = (
        P("rows", None),
        P("rows"),
        P(),
        P("rows"),
        P("rows", None),
        P("rows"),
        P("section", None),
        P("section", None, "rows"),
        P("section", None, "rows"),
        P("section", "rows", None),
        P(),
        P(),
        P("rows"),
    )
    return jax.shard_map(
        on_device,
        mesh=mesh,
        in_specs=placed,
        out_specs=(P(("rows", "section")), P(("rows", "section"))),
        check_vma=False,
    )
```

```python
import functools

import jax
import jax.numpy as jnp
from jax import lax
from jax.experimental import pallas as pl
from jax.experimental.pallas import tpu as pltpu
from jax.sharding import PartitionSpec as P

MESH = pl.DeviceIdType.MESH
MICRO = 16
SLOTS = 17
GROUP = 8
OWN = 560
SPAN = 1152
TABLE = 4096
EARLY = 12


def place(member, half):
    y = member // 2
    return 4 * y + 2 * (member % 2) + (y + half) % 2


def copy_to(src, dst, send, recv, section, rows):
    return pltpu.make_async_remote_copy(
        src_ref=src,
        dst_ref=dst,
        send_sem=send,
        recv_sem=recv,
        device_id={"section": section, "rows": rows},
        device_id_type=MESH,
    )


FIRST = (((0,), (0,)), ((), ()))


def take(ref, sem):
    pltpu.make_async_copy(ref, ref, sem).wait()


PIECES = ((0, 144), (144, 144), (288, 144), (432, 128))
GATHER_ORDER = ((2, 1), (1, 0), (3, 0), (1, 1), (3, 1), (0, 1), (2, 0))
SCATTER_ORDER = ((2, 0), (2, 1), (1, 1), (3, 1), (1, 0), (3, 0), (0, 0), (0, 1))


def model_kernel(
    features,
    ages,
    age_table,
    returns,
    owners,
    slots,
    gain_in,
    wg_in,
    wu_in,
    wd_in,
    final_gain,
    head,
    old,
    out_rewards,
    out_weights,
    wg_rows,
    wu_rows,
    wg,
    wu,
    wd,
    gain,
    x0,
    xs,
    ag,
    rs,
    ps,
    hid,
    news,
    allrew,
    told,
    sums,
    cols,
    shares,
    bests,
    given,
    own_sem,
    w0_send,
    w0_recv,
    w1_send,
    w1_recv,
    x_send,
    x_recv,
    ag_send,
    ag_recv,
    rs_send,
    rs_recv,
    all_send,
    all_recv,
    told_send,
    told_recv,
    sum_send,
    sum_recv,
):
    section = lax.axis_index("section")
    rows = lax.axis_index("rows")
    plane, core = section // 2, section % 2
    y, x = rows // 4, rows % 4
    half = (x + y) % 2
    stage = 2 * plane + half
    member = y * 2 + x // 2
    primary = core == half
    sibling = 2 * plane + 1 - core
    last = stage == 7
    later_half = 1 - half
    later_section = jnp.where(half == 0, section, (section + 2) % 8)
    base = jnp.where(last, SLOTS, 0)
    blocks = MICRO - 1 + 2 * core
    across_section = 2 * ((plane + half + half + 3) % 4) + core
    width = features.shape[-1]
    r = features.shape[0] // MICRO
    block = GROUP * r

    def peer_of(dy, db):
        return 2 * ((y + dy) % 4) + (member + db) % 2

    barrier = pltpu.get_barrier_semaphore()

    def greet(to_section, to_rows):
        pl.semaphore_signal(
            barrier,
            inc=1,
            device_id={"section": to_section, "rows": to_rows},
            device_id_type=MESH,
        )

    for step in range(1, 16):
        greet(section, (rows + step) % 16)
    greet(sibling, rows)
    for k in range(GROUP):
        greet(across_section, place(k, 1 - half))
    near = (
        4 * y + (x + 1) % 4,
        4 * y + (x + 3) % 4,
        4 * ((y + 1) % 4) + x,
        4 * ((y + 3) % 4) + x,
    )

    def own_copies():
        return (
            pltpu.make_async_copy(gain_in, gain, own_sem.at[0]),
            pltpu.make_async_copy(wg_in, wg_rows.at[pl.ds(0, OWN)], own_sem.at[1]),
            pltpu.make_async_copy(wu_in, wu_rows.at[pl.ds(0, OWN)], own_sem.at[2]),
            pltpu.make_async_copy(wd_in, wd.at[pl.ds(0, OWN)], own_sem.at[3]),
        )

    def other_copies():
        return [
            pltpu.make_async_copy(src, given.at[i], own_sem.at[i + 1])
            for i, src in enumerate((wg_in, wu_in, wd_in))
        ]

    def sibling_copies():
        pairs = (
            (gain, gain),
            (wg_rows.at[pl.ds(0, OWN)], wg_rows.at[pl.ds(0, OWN)]),
            (wu_rows.at[pl.ds(0, OWN)], wu_rows.at[pl.ds(0, OWN)]),
            (wd.at[pl.ds(0, OWN)], wd.at[pl.ds(0, OWN)]),
        )
        return [
            copy_to(src, dst, w0_send.at[i], w0_recv.at[i], sibling, rows)
            for i, (src, dst) in enumerate(pairs)
        ]

    def piece_copies(n, to_section, to_rows, relay):
        at, size = PIECES[n]
        targets = [ref.at[pl.ds(OWN + at, size)] for ref in (wg_rows, wu_rows, wd)]
        sources = targets if relay else [given.at[i, pl.ds(at, size)] for i in range(3)]
        return [
            copy_to(src, dst, w1_send.at[i, n], w1_recv.at[i, n], to_section, to_rows)
            for i, (src, dst) in enumerate(zip(sources, targets))
        ]

    gather_rows = [place(peer_of(dy, db), half) for dy, db in GATHER_ORDER]
    scatter_peers = [peer_of(dy, db) for dy, db in SCATTER_ORDER]
    scatter_rows = [place(peer, later_half) for peer in scatter_peers]

    def feed(part):
        return copy_to(
            x0.at[pl.ds(4 * part, 4)],
            xs.at[pl.ds(4 * part, 4)],
            x_send.at[part],
            x_recv.at[part],
            1,
            place(member, 0),
        )

    feeding = jnp.logical_and(section == 7, half == 1)
    entering = jnp.logical_and(section == 0, half == 0)
    fed = jnp.logical_and(section == 1, half == 0)

    @pl.when(primary)
    def _():
        for copy in own_copies():
            copy.start()

    @pl.when(jnp.logical_not(primary))
    def _():
        for copy in other_copies():
            copy.start()

    @pl.when(entering | feeding | fed)
    def _():
        number = age_table.shape[0]
        level = lax.broadcasted_iota(jnp.int32, (number, features.shape[0]), 0)
        onehot = (level == ages[...]).astype(jnp.float32).astype(jnp.bfloat16)
        aged = lax.dot_general(onehot, age_table[...], FIRST, preferred_element_type=jnp.float32)
        entry = (features[...].astype(jnp.float32) + aged).reshape(MICRO, r, width)
        x0[...] = entry.astype(jnp.bfloat16)

        @pl.when(entering)
        def _():
            xs[pl.ds(0, MICRO)] = x0[...]

        @pl.when(fed)
        def _():
            xs[MICRO] = x0[MICRO - 1]

    tail = pl.ds(2 * OWN, SPAN - 2 * OWN)
    for ref in (wg_rows, wu_rows, wd):
        ref[tail, :] = jnp.zeros((SPAN - 2 * OWN, width), jnp.bfloat16)
    news[...] = (owners[...] * TABLE + slots[...]).astype(jnp.float32)
    told[rows, 0] = returns[...]
    told[rows, 1] = news[...]

    pl.semaphore_wait(barrier, 24)

    @pl.when(jnp.logical_not(primary))
    def _():
        for i, copy in enumerate(other_copies()):
            copy.wait()
            for n in range(4):
                piece_copies(n, section, near[n], False)[i].start()

    @pl.when(feeding)
    def _():
        for part in range(4):
            feed(part).start()

    @pl.when(primary)
    def _():
        for own, copy in zip(own_copies(), sibling_copies()):
            own.wait()
            copy.start()

    def enter(m):
        @pl.when(fed & (m % 4 == 0) & (m < MICRO))
        def _():
            take(xs.at[pl.ds(m, 4)], x_recv.at[m // 4])

        @pl.when(stage > 0)
        def _():
            xs[m] = summed(m)

        wide = xs[m].astype(jnp.float32)
        mean = jnp.mean(wide * wide, axis=-1, keepdims=True)
        ag[m, member] = (wide * lax.rsqrt(mean + 1e-06) * gain[...]).astype(jnp.bfloat16)
        for to_rows in gather_rows:
            copy_to(
                ag.at[m, member], ag.at[m, member], ag_send.at[m], ag_recv.at[m], section, to_rows
            ).start()

    def summed(m):
        take(rs.at[m], rs_recv.at[m])
        total = rs[m, 0].astype(jnp.float32)
        for i in range(1, GROUP):
            total = total + rs[m, i].astype(jnp.float32)
        return total.astype(jnp.bfloat16)

    def layer(m):
        take(ag.at[m, pl.ds(0, GROUP - 1)], ag_recv.at[m])
        normed = ag[m].reshape(block, width)
        for at in range(0, SPAN, 256):
            size = min(256, SPAN - at)
            gate = jnp.dot(normed, wg[:, at : at + size], preferred_element_type=jnp.float32)
            upper = jnp.dot(normed, wu[:, at : at + size], preferred_element_type=jnp.float32)
            hid[:, at : at + size] = (gate * jax.nn.sigmoid(gate) * upper).astype(jnp.bfloat16)
        to_section = jnp.where(last & (m >= EARLY), section, later_section)
        ours = lax.broadcasted_iota(jnp.int32, (GROUP, r, 256), 0) == member
        for at in range(0, width, 256):
            part = jnp.dot(hid[...], wd[:, at : at + 256], preferred_element_type=jnp.float32)
            kept = xs[m, :, at : at + 256].astype(jnp.float32)[None]
            part = part.reshape(GROUP, r, 256) + jnp.where(ours, kept, 0.0)
            ps[m, :, :, at : at + 256] = part.astype(jnp.bfloat16)
            if at + 256 in (width // 2, width):
                span = pl.ds(at + 256 - width // 2, width // 2)
                for peer, to_rows in zip(scatter_peers, scatter_rows):
                    copy_to(
                        ps.at[m, peer, :, span],
                        rs.at[base + m, member, :, span],
                        rs_send.at[m],
                        rs_recv.at[base + m],
                        to_section,
                        to_rows,
                    ).start()

    def turned(source, target):
        def turn(i, carry):
            at = pl.multiple_of(i * 128, 128)
            target[:, pl.ds(at, 128)] = source[pl.ds(at, 128), :].T
            return carry

        lax.fori_loop(0, SPAN // 128, turn, 0)

    @pl.when(jnp.logical_not(primary))
    def _():
        sibling_copies()[0].wait_recv()

    begun = jnp.where(stage == 0, 1, 0)

    def early(m, carry):
        enter(m)
        return carry

    lax.fori_loop(0, begun, early, 0)

    for step in range(1, 16):
        copy_to(
            told.at[rows],
            told.at[rows],
            told_send,
            told_recv,
            section,
            (rows + step) % 16,
        ).start()

    @pl.when(jnp.logical_not(primary))
    def _():
        for copy in sibling_copies()[1:]:
            copy.wait_recv()

    for i in range(3):
        for n in range(4):

            @pl.when(primary)
            def _():
                copy = piece_copies(n, sibling, rows, True)[i]
                copy.wait_recv()
                copy.start()

            @pl.when(jnp.logical_not(primary))
            def _():
                piece_copies(n, section, near[n], False)[i].wait_recv()

        if i < 2:
            turned((wg_rows, wu_rows)[i], (wg, wu)[i])

    share = TABLE // 8
    parts = share // 128
    lane = lax.broadcasted_iota(jnp.int32, (8, 128), 1)
    sub = lax.broadcasted_iota(jnp.int32, (8, 128), 0)
    first = rows * TABLE + section * share
    mine = section * 16 + rows
    side = section % 2

    def before(q):
        near_old = old[pl.ds(pl.multiple_of(8 * (section // 2), 8), 8), :]
        return jnp.where(side == 0, near_old[q : q + 1], near_old[q + parts : q + parts + 1])

    def lines():
        wide = [jnp.broadcast_to(told[j, 1], (8, 128)) for j in range(16)]
        return wide + [(first + q * 128 + lane).astype(jnp.float32) for q in range(parts)]

    def column(line, m):
        picked = jnp.where(lane == m * r + sub, jnp.broadcast_to(line, (8, 128)), 0.0)
        return jnp.broadcast_to(jnp.sum(picked, axis=1, keepdims=True), (8, 128))

    def prepare():
        take(told.at[pl.ds(0, 15)], told_recv)
        names = lines()

        def count(j, totals):
            for m in range(MICRO):
                col = column(told[j, 1], m)
                cols[j, m] = col
                totals = [t + jnp.where(col == name, 1.0, 0.0) for t, name in zip(totals, names)]
            return totals

        zeros = [jnp.zeros((8, 128), jnp.float32)] * len(names)
        totals = lax.fori_loop(0, 16, count, zeros)
        counts = [jnp.sum(t, axis=0, keepdims=True) for t in totals]
        for j in range(16):
            shares[j] = 1.0 / counts[j]
        rest = jnp.zeros((1, 128), jnp.float32)
        for q in range(parts):
            rest = rest + jnp.where(counts[16 + q] > 0.0, 0.0, before(q))
        sums[mine] = jnp.broadcast_to(jnp.sum(rest, axis=1, keepdims=True), (1, 128))

    @pl.when(stage > 3)
    def _():
        prepare()

    def tick(m, carry):
        start = jnp.maximum(m + jnp.where(m > 0, 1, 0), begun) + jnp.where((stage == 0) & (m > 0), 1, 0)
        stop = jnp.minimum(m + jnp.where(stage == 0, 3, 2), blocks)
        lax.fori_loop(start, stop, early, 0)
        layer(m)
        return carry

    lax.fori_loop(0, blocks, tick, 0)

    @pl.when(stage < 4)
    def _():
        prepare()

    shard = place(member, core)
    finals = (stage == 0, stage == 6)

    def everyone(ref, send, recv):
        targets = [2 * ((plane + away) % 4) + side for away in (2, 1, 3, 0) for side in (1 - core, core)]

        def send_row(step, carry):
            to_rows = lax.rem(rows + step, 16)
            for to_section in targets:
                copy_to(ref, ref, send, recv, to_section, to_rows).start()
            return carry

        lax.fori_loop(1, 16, send_row, 0)
        for to_section in targets[:-1]:
            copy_to(ref, ref, send, recv, to_section, rows).start()

    def rewarded(m, line, at):
        wide = summed(SLOTS + m).astype(jnp.float32)
        mean = jnp.mean(wide * wide, axis=-1, keepdims=True)
        ready = wide * lax.rsqrt(mean + 1e-06) * final_gain[...].reshape(1, width)
        value = jnp.sum(ready * head[...].reshape(1, width), axis=-1, keepdims=True)
        return line + jnp.where(lane == at * r + sub, value, 0.0)

    def finish(m, line):
        return rewarded(m, line, m)

    def share_rewards(turn, start, stop):
        @pl.when(finals[turn])
        def _():
            empty = jnp.zeros((r, 128), jnp.float32)
            line = lax.fori_loop(start, stop, finish, empty)
            allrew[turn, shard, 0] = jnp.sum(line, axis=0, keepdims=True)
            allrew[turn, shard, 1] = jnp.zeros((1, 128), jnp.float32)
            if turn:

                @pl.when(core == 1)
                def _():
                    spare = rewarded(MICRO, empty, MICRO - 1)
                    allrew[turn, shard, 1] = jnp.sum(spare, axis=0, keepdims=True)

            everyone(allrew.at[turn, shard], all_send.at[turn], all_recv.at[turn])

    def await_rewards(turn):
        @pl.when(finals[turn])
        def _():
            take(allrew.at[turn, pl.ds(0, 15)], all_recv.at[turn])

        @pl.when(jnp.logical_not(finals[turn]))
        def _():
            take(allrew.at[turn], all_recv.at[turn])

    def priority(turn, j):
        line = allrew[turn, j, 0]
        if turn and (j // 4 + j) % 2 == 0:
            line = line + allrew[turn, j ^ 1, 1]
        gap = jnp.abs(line - told[j, 0]) + 0.05
        return jnp.exp(0.6 * jnp.log(gap))

    def largest(best, names, line, j, m):
        col, value = cols[j, m], column(line, m)
        return [jnp.maximum(b, jnp.where(col == n, value, 0.0)) for b, n in zip(best, names)]

    share_rewards(0, 0, EARLY)
    await_rewards(0)
    everyone(sums.at[mine], sum_send, sum_recv)
    names = lines()

    def first_round(j, best):
        line = priority(0, j)
        for m in range(EARLY):
            best = largest(best, names, line, j, m)
        return best

    best = lax.fori_loop(0, 16, first_round, [jnp.zeros((8, 128), jnp.float32)] * len(names))
    for i, b in enumerate(best):
        bests[i] = b
    share_rewards(1, EARLY, MICRO - 1 + core)

    def drained(m, carry):
        take(ag.at[m, pl.ds(0, GROUP - 1)], ag_send.at[m])
        take(rs.at[m], rs_send.at[m])
        return carry

    lax.fori_loop(0, blocks, drained, 0)
    take(told.at[pl.ds(0, 15)], told_send)

    @pl.when(feeding)
    def _():
        for part in range(4):
            feed(part).wait_send()

    @pl.when(primary)
    def _():
        for copy in sibling_copies():
            copy.wait_send()
        for n in range(4):
            for copy in piece_copies(n, sibling, rows, True):
                copy.wait_send()

    @pl.when(jnp.logical_not(primary))
    def _():
        for n in range(4):
            for copy in piece_copies(n, section, near[n], False):
                copy.wait_send()

    take(sums.at[pl.ds(0, 127)], sum_send)
    take(sums.at[pl.ds(0, 127)], sum_recv)
    whole = jnp.sum(sums[...], axis=0)

    await_rewards(1)
    names = lines()
    best = [bests[i] for i in range(len(names))]
    for j in range(16):
        line = priority(1, j)
        for m in range(EARLY, MICRO):
            best = largest(best, names, line, j, m)
    best = [jnp.max(b, axis=0, keepdims=True) for b in best]
    named = jnp.zeros((1, 128), jnp.float32)
    for j in range(16):
        named = named + best[j] * shares[j]
    whole = whole + jnp.sum(named, axis=1, keepdims=True)
    for q in range(parts):
        fresh = jnp.where(best[16 + q] > 0.0, best[16 + q], before(q))
        out_weights[q : q + 1, :] = fresh * (float(16 * TABLE) / whole)
    spots = lax.broadcasted_iota(jnp.int32, (1, 128), 1)
    spare = jnp.where(half == 0, allrew[1, rows + 1 - 2 * (rows % 2), 1], 0.0)
    out_rewards[...] = jnp.where(spots < EARLY * r, allrew[0, rows, 0], allrew[1, rows, 0] + spare)

    for turn in range(2):

        @pl.when(finals[turn])
        def _():
            def sent(step, carry):
                take(allrew.at[turn], all_send.at[turn])
                return carry

            lax.fori_loop(0, 7, sent, 0)
            take(allrew.at[turn, pl.ds(0, 15)], all_send.at[turn])


def on_device(
    features,
    ages,
    age_table,
    returns,
    owners,
    slots,
    norm_gain,
    w_gate,
    w_up,
    w_down,
    final_gain,
    reward_head,
    old_priority,
):
    sections = lax.axis_size("section")
    section = lax.axis_index("section")
    rows_here, width = features.shape
    r = rows_here // MICRO
    vmem = pl.BlockSpec(memory_space=pltpu.VMEM)
    hbm = pl.BlockSpec(memory_space=pl.ANY)
    dma = pltpu.SemaphoreType.DMA
    half, single = jnp.bfloat16, jnp.float32
    line, weights = pl.pallas_call(
        model_kernel,
        out_shape=[
            jax.ShapeDtypeStruct((1, rows_here), single),
            jax.ShapeDtypeStruct((TABLE // sections // 128, 128), single),
        ],
        in_specs=[vmem] * 6 + [hbm] * 4 + [vmem] * 3,
        out_specs=[vmem] * 2,
        scratch_shapes=[
            pltpu.VMEM((SPAN, width), half),
            pltpu.VMEM((SPAN, width), half),
            pltpu.VMEM((width, SPAN), half),
            pltpu.VMEM((width, SPAN), half),
            pltpu.VMEM((SPAN, width), half),
            pltpu.VMEM((1, width), single),
            pltpu.VMEM((MICRO, r, width), half),
            pltpu.VMEM((SLOTS, r, width), half),
            pltpu.VMEM((SLOTS, GROUP, r, width), half),
            pltpu.VMEM((2 * SLOTS, GROUP, r, width), half),
            pltpu.VMEM((SLOTS, GROUP, r, width), half),
            pltpu.VMEM((GROUP * r, SPAN), half),
            pltpu.VMEM((1, 128), single),
            pltpu.VMEM((2, 16, 2, 1, 128), single),
            pltpu.VMEM((16, 2, 1, 128), single),
            pltpu.VMEM((128, 1, 128), single),
            pltpu.VMEM((16, MICRO, 8, 128), single),
            pltpu.VMEM((16, 1, 128), single),
            pltpu.VMEM((16 + TABLE // sections // 128, 8, 128), single),
            pltpu.VMEM((3, OWN, width), half),
            dma((4,)),
            dma((4,)),
            dma((4,)),
            dma((3, 4)),
            dma((3, 4)),
            dma((4,)),
            dma((4,)),
            dma((SLOTS,)),
            dma((SLOTS,)),
            dma((SLOTS,)),
            dma((2 * SLOTS,)),
            dma((2,)),
            dma((2,)),
            dma,
            dma,
            dma,
            dma,
        ],
        compiler_params=pltpu.CompilerParams(
            collective_id=0, has_side_effects=True, vmem_limit_bytes=60 * 1024 * 1024
        ),
        name="reward_model",
    )(
        features,
        ages.reshape(1, rows_here),
        age_table,
        returns.reshape(1, rows_here),
        owners.reshape(1, rows_here),
        slots.reshape(1, rows_here),
        norm_gain,
        w_gate[0].T,
        w_up[0].T,
        w_down[0],
        final_gain,
        reward_head,
        old_priority.reshape(TABLE // 128, 128),
    )
    part = rows_here // sections

    def hand_over(line_ref, weights_ref, rewards_out, weights_out):
        turned = pltpu.roll(line_ref[...], (rows_here - section_of() * part) % rows_here, 1)
        rewards_out[...] = turned[:, :part]
        weights_out[...] = weights_ref[...]

    def section_of():
        return lax.axis_index("section")

    rewards, weights = pl.pallas_call(
        hand_over,
        out_shape=[
            jax.ShapeDtypeStruct((1, part), single),
            jax.ShapeDtypeStruct(weights.shape, single),
        ],
        in_specs=[vmem] * 2,
        out_specs=[vmem] * 2,
        name="hand_over",
    )(line, weights)
    return (rewards.reshape(-1), weights.reshape(-1))


def solution(mesh):
    placed = (
        P("rows", None),
        P("rows"),
        P(),
        P("rows"),
        P("rows", None),
        P("rows"),
        P("section", None),
        P("section", None, "rows"),
        P("section", None, "rows"),
        P("section", "rows", None),
        P(),
        P(),
        P("rows"),
    )
    return jax.shard_map(
        on_device,
        mesh=mesh,
        in_specs=placed,
        out_specs=(P(("rows", "section")), P(("rows", "section"))),
        check_vma=False,
    )
```
